32 devices in a mesh: section: 16 (over z, y, x), tensor: 2 (over core).
Axes of the slice: x: 2, y: 2, z: 4, core: 2. Of those that a mesh axis runs over, the one named last changes fastest.
Arguments:
- hidden_in: bfloat16 [128, 8192], P(None, 'tensor'), may hold values from -36 to 36
- segment_ids: int32 [4, 32], replicated, may hold values from 0 to 7, never falling along the last dimension, each value on 1 to 8 neighbouring positions
- segment_job: int32 [4, 8], replicated, may hold values from 0 to 5
- job_adapter: int32 [6], replicated, may hold values from 0 to 3
- owner: int32 [16], P('section'), may hold values from 0 to 1
- frozen: bfloat16 [16, 8192, 4096], P('section', None, 'tensor'), may hold values from -0.0625 to 0.0625
- norm_gain: bfloat16 [16, 4096], P('section'), may hold values from 0.3984375 to 1.59375
- inbox_down: bfloat16 [16, 2, 4096, 128], P('section', 'tensor'), may hold values from -0.0625 to 0.0625
- inbox_up: bfloat16 [16, 2, 128, 4096], P('section', 'tensor'), may hold values from -1 to 1
Outputs:
- section_out: bfloat16 [16, 128, 4096], P('section', None, 'tensor')
The draws below stay inside these ranges and needn't reach their ends.
Inputs may be any that keep to these rules, and one draw needn't show every extreme that they name: `segment_ids`: within each micro-batch the segment numbers never fall, and each of the 8 segments has 1 to 8 tokens.
All inputs are finite; a program needn't handle non-finite values.
Results may differ from the reference program's by a relative error of at most 0.02.
Values may be sent and summed in bfloat16 or wider, within the bound.
A program may use at most 128 MiB of HBM per device.

```python
import math
import jax
import jax.numpy as jnp
import numpy as np
from jax import lax

D = 8192
R = 32
NEW = 4
JOBS = 6
MB = 4
MTOK = 32
SEGS = 8
TOK = 128
PIECE = 2048
SEG_MOST = 8
N_SECTION = 16
N_TENSOR = 2


def draw_hidden_in(key, part):
    base_key, col_key, row_key = jax.random.split(key, 3)
    col_scale = jnp.exp(jax.random.uniform(col_key, (1, D), jnp.float32, math.log(0.3), math.log(3.0)))
    row_scale = jnp.exp(jax.random.uniform(row_key, (TOK, 1), jnp.float32, math.log(0.3), math.log(3.0)))
    values = jnp.clip(jax.random.normal(base_key, (TOK, D), jnp.float32), -4.0, 4.0)
    return (values * col_scale * row_scale).astype(jnp.bfloat16)


def place_ends(result, stream_key, smallest, top_value):
    dims = result.shape
    index_at = [jax.random.randint(jax.random.fold_in(stream_key, axis), (), 0, dims[axis]) for axis in range(len(dims))]
    result = result.at[tuple(index_at)].set(smallest)
    longest = dims.index(max(dims))
    index_at[longest] = (index_at[longest] + 1) % dims[longest]
    return result.at[tuple(index_at)].set(top_value)


def steps_of(key, shape, shards, low, largest):
    def one(position, shards_of):
        draws = jax.random.uniform(jax.random.fold_in(jax.random.fold_in(key, 6), position), (shards_of,), jnp.float32, low / len(shards), largest / len(shards))
        return jnp.repeat(jnp.exp(draws), shape[position] // shards_of).reshape((-1,) + (1,) * (len(shape) - position - 1))

    loudness = one(*shards[0])
    for cut in shards[1:]:
        loudness = loudness * one(*cut)
    return loudness


def split_up(amount, total, reach, lean):
    weights = [(1 << 20) // math.isqrt(standing ** lean) + 1 for standing in range(2, amount + 1)]
    rest, holding = total - reach - (amount - 1), [1] * (amount - 1)
    while rest > 0:
        free = [i for i in range(amount - 1) if holding[i] < reach]
        whole, budget = sum([weights[i] for i in free]), rest
        for i in free:
            extra = min(reach - holding[i], max(1, budget * weights[i] // whole), rest)
            holding[i] = holding[i] + extra
            rest = rest - extra
    return np.array([reach] + holding)


def uneven_parts(stream_key, count, total, most, skew):
    if count == 2:
        one = jax.random.randint(stream_key, (), max(1, total - most), min(most, total - 1) + 1)
        return jnp.stack([one, total - one])
    lengths = jnp.asarray(split_up(count, total, most, skew), jnp.int32)
    couples = (count - 1) // 2
    giver, taker = lengths[1:1 + 2 * couples:2], lengths[2:2 + 2 * couples:2]
    room = jnp.minimum(giver - 1, most - taker)
    passed = jax.random.randint(jax.random.fold_in(stream_key, 1), (couples,), 0, 1 << 20) % (room + 1)
    lengths = lengths.at[1:1 + 2 * couples:2].set(giver - passed).at[2:2 + 2 * couples:2].set(taker + passed)
    return lengths[jax.random.permutation(jax.random.fold_in(stream_key, 2), count)]


def gaussian(stream_key, shape, scale, reach, cuts=(), kind=jnp.bfloat16):
    loudness = steps_of(stream_key, shape, cuts, -0.22, 0.18) if cuts else 1.0
    result = jax.random.normal(stream_key, shape, jnp.float32) * scale * loudness
    return jnp.minimum(jnp.maximum(result, -reach), reach).astype(kind)


def setup_inputs(seed: int = 0) -> dict:
    key_list = jax.random.split(jax.random.key(seed), 10)
    hidden_in = draw_hidden_in(jax.random.fold_in(key_list[9], 71), 0)
    segment_ids = jax.vmap(lambda own: jnp.searchsorted(jnp.cumsum(uneven_parts(own, SEGS, MTOK, SEG_MOST, 2)), jnp.arange(MTOK), side="right"))(jax.random.split(key_list[1], MB)).reshape((MB, MTOK)).astype(jnp.int32)
    segment_job = place_ends(jax.random.randint(key_list[2], (MB, SEGS), 0, JOBS), jax.random.fold_in(key_list[2], 1), 0, JOBS - 1).astype(jnp.int32)
    job_adapter = place_ends(jax.random.randint(key_list[3], (JOBS,), 0, NEW), jax.random.fold_in(key_list[3], 1), 0, NEW - 1).astype(jnp.int32)
    owner = place_ends(jax.random.randint(key_list[4], (N_SECTION,), 0, N_TENSOR), jax.random.fold_in(key_list[4], 1), 0, N_TENSOR - 1).astype(jnp.int32)
    frozen = gaussian(key_list[5], (N_SECTION, D, D // 2), D ** -0.5, 0.0625, ((0, 16), (2, 2)))
    norm_gain = jnp.clip(1.0 + 0.12 * jax.random.normal(key_list[6], (N_SECTION, D // 2), jnp.float32), 0.3984375, 1.59375).astype(jnp.bfloat16)
    inbox_down = gaussian(key_list[7], (N_SECTION, N_TENSOR, D // 2, NEW * R), D ** -0.5, 0.0625, ((0, 16), (1, 2)))
    inbox_up = gaussian(key_list[8], (N_SECTION, N_TENSOR, NEW * R, D // 2), R ** -0.5, 1.0, ((0, 16), (1, 2)))
    return dict(hidden_in=hidden_in, segment_ids=segment_ids, segment_job=segment_job, job_adapter=job_adapter, owner=owner, frozen=frozen, norm_gain=norm_gain, inbox_down=inbox_down, inbox_up=inbox_up)


epsilon = 1e-05

def alternate(lower_part, upper_part):
    lead_rows = lower_part.shape[0]
    blocks = jnp.stack([lower_part.reshape(lead_rows, N_TENSOR, PIECE), upper_part.reshape(lead_rows, N_TENSOR, PIECE)], axis=2)
    return blocks.reshape(lead_rows, 2 * N_TENSOR * PIECE)

def product(left, right):
    return jnp.dot(left, right, preferred_element_type=jnp.float32)

def reference(hidden_in, segment_ids, segment_job, job_adapter, owner, frozen, norm_gain, inbox_down, inbox_up):
    token_job = jnp.take_along_axis(segment_job, segment_ids, axis=1)
    token_adapter = jnp.take(job_adapter, token_job.reshape(TOK), axis=0)
    keep_mask = jnp.arange(NEW * R, dtype=jnp.int32)[None, :] // R == token_adapter[:, None]
    state_now = hidden_in
    pieces = []
    for section_level in range(N_SECTION // 2):
        low_index = 2 * section_level
        high_index = low_index + 1
        weight = alternate(frozen[low_index], frozen[high_index])
        down_rows = alternate(inbox_down[low_index, owner[low_index]].T, inbox_down[high_index, owner[high_index]].T).T
        up_cols = alternate(inbox_up[low_index, owner[low_index]], inbox_up[high_index, owner[high_index]])
        gain_row = alternate(norm_gain[low_index][None, :], norm_gain[high_index][None, :])[0]
        values = state_now.astype(jnp.float32)
        row_scale = lax.rsqrt(lax.optimization_barrier(jnp.mean(values * values, axis=1, keepdims=True)) + epsilon)
        normed = (values * row_scale * gain_row.astype(jnp.float32)).astype(jnp.bfloat16)
        projected = product(normed, down_rows)
        kept_rank = jnp.where(keep_mask, projected, 0.0).astype(jnp.bfloat16)
        state_now = (values + product(normed, weight) + product(kept_rank, up_cols)).astype(jnp.bfloat16)
        split_state = state_now.reshape(TOK, N_TENSOR, 2, PIECE)
        pieces.append(split_state[:, :, 0, :].reshape(TOK, N_TENSOR * PIECE))
        pieces.append(split_state[:, :, 1, :].reshape(TOK, N_TENSOR * PIECE))
    return jnp.stack(pieces, axis=0)
```

```python
import functools
import jax
import jax.numpy as jnp
from jax import lax
from jax.experimental import pallas as pl
from jax.experimental.pallas import tpu as pltpu
from jax.sharding import PartitionSpec as P

R = 32
TILE = 256
MESH = pl.DeviceIdType.MESH
epsilon = 1e-05
f32, bf16 = jnp.float32, jnp.bfloat16


def run(steps):
    products = [step for step in steps if isinstance(step, list)]

    def push(n):
        if n < len(products):
            for q, (rhs, _, _) in enumerate(products[n]):
                pltpu.matmul_push_rhs(rhs(), staging_register=n % 2, mxu_index=q)

    push(0)
    push(1)
    n = 0
    for step in steps:
        if isinstance(step, list):
            for _, acc, lhs in step:
                pltpu.matmul_acc_lhs(acc, lhs(), load_staged_rhs=n % 2)
            push(n + 2)
            n += 1
        else:
            step()


def kernel(
    sections, tensors, units, rows, piece, chunks, quarters, ranks, jobs_of,
    hidden, ids, seg_job, job_ad, owner, frozen, gain, idown, iup,
    out,
    w, x0, xg0, xbuf, outbuf, gother, dbuf, ubuf, dsel, usel, lowbuf, mask, kept0,
    wsem, hidsem, hidsend, dsem, usem, isend, gsem, ysem, xsem, psem, lsem,
    osend, xsend, fsend, lsend, wout,
):
    levels = sections // 2
    step = piece // chunks
    tokens = units * rows
    full = 2 * tensors * piece
    depth = full // quarters
    inner = step // TILE
    tiles = piece // TILE
    segs, jobs = jobs_of
    s = lax.axis_index("section")
    t = lax.axis_index("tensor")
    h = lax.rem(s, 2)
    level = s // 2
    other = s + 1 - 2 * h
    b = 2 * t + h
    last = level == levels - 1

    def peer(d):
        return lax.rem(t + d, tensors)

    def at(start, size):
        return pl.ds(pl.multiple_of(start, TILE), size)

    def part(k):
        return at(k * piece, piece)

    def remote(src, dst, send, recv, section, tensor):
        return pltpu.make_async_remote_copy(
            src_ref=src, dst_ref=dst, send_sem=send, recv_sem=recv,
            device_id=(section, tensor), device_id_type=MESH,
        )

    def landed(ref, sem):
        pltpu.make_async_copy(ref, ref, sem).wait()

    def unit_rows(m):
        return pl.ds(pl.multiple_of(m * rows, rows), rows)

    own_hidden = pltpu.make_async_copy(hidden, x0.at[t], hidsem.at[t])
    own_down = pltpu.make_async_copy(idown.at[0, 0, part(t), :], dbuf.at[t], dsem.at[t])
    own_up = pltpu.make_async_copy(iup.at[0, 0, :, part(t)], ubuf.at[t], usem.at[t])

    def weight_cols(j, k):
        here = (at(k * depth, depth), at(j * step, step))
        return pltpu.make_async_copy(frozen.at[(0,) + here], w.at[here], wsem.at[j, k])

    def weight_rows(j, k):
        share = depth // chunks
        here = at((k * chunks + j) * share, share)
        return pltpu.make_async_copy(frozen.at[0, here, :], w.at[here, :], wsem.at[j, k])

    @pl.when(level == 0)
    def _():
        own_hidden.start()

    own_down.start()
    own_up.start()

    @pl.when(level == 0)
    def _():
        for j in range(chunks):
            for k in range(quarters):
                weight_cols(j, k).start()

    @pl.when(level > 0)
    def _():
        for j in range(chunks):
            for k in range(quarters):
                weight_rows(j, k).start()

    barrier = pltpu.get_barrier_semaphore()

    def greet(section, tensor):
        pl.semaphore_signal(barrier, inc=1, device_id=(section, tensor), device_id_type=MESH)

    for d in range(1, tensors):
        greet(s, peer(d))
    for d in range(tensors):
        greet(other, peer(d))

    @pl.when(level > 0)
    def _():
        greet(s - 2, t)

    @pl.when(level < levels - 1)
    def _():
        greet(s + 2, t)

    ends = (level > 0).astype(jnp.int32) + (level < levels - 1).astype(jnp.int32)
    pl.semaphore_wait(barrier, 2 * tensors - 1 + ends)

    def send_hidden(d):
        return remote(hidden, x0.at[t], hidsend.at[d], hidsem.at[t], s, peer(d))

    def send_down(d):
        return remote(idown.at[0, 0, part(peer(d)), :], dbuf.at[t], isend.at[0, d], dsem.at[t], s, peer(d))

    def send_up(d):
        return remote(iup.at[0, 0, :, part(peer(d))], ubuf.at[t], isend.at[1, d], usem.at[t], s, peer(d))

    send_gain = remote(gain, gother, gsem.at[0], gsem.at[1], other, t)
    send_gain.start()

    @pl.when(level == 0)
    def _():
        for d in range(1, tensors):
            send_hidden(d).start()

    for d in range(1, tensors):
        send_down(d).start()
        send_up(d).start()

    def send_out(m, c):
        return remote(outbuf.at[m, c], xbuf.at[m, b, c], osend.at[m], ysem.at[m, c], s + 2, t)

    def write_out(m, c):
        return pltpu.make_async_copy(outbuf.at[m, c], out.at[0, unit_rows(m), at(c * step, step)], wout.at[m])

    def low_sends(slot, ref):
        for side in range(2):
            for d in range(1 - side, tensors):
                remote(ref, ref, lsend.at[slot], lsem.at[slot, b], s if side == 0 else other, peer(d)).start()

    def low_blocks():
        return [2 * peer(d) + (h if side == 0 else 1 - h) for side in range(2) for d in range(1 - side, tensors)]

    for m in range(units):
        seg = ids[pl.ds(m, 1), :]
        slot = jnp.zeros_like(seg)
        for g in range(segs):
            slot = jnp.where(seg == g, job_ad[seg_job[m, g]], slot)
        eye = lax.broadcasted_iota(jnp.int32, (rows, rows), 0) == lax.broadcasted_iota(jnp.int32, (rows, rows), 1)
        spread = jnp.where(eye, jnp.broadcast_to(slot.astype(f32), (rows, rows)), 0.0)
        column = jnp.sum(spread, axis=1, keepdims=True)
        rank = lax.broadcasted_iota(jnp.int32, (rows, ranks), 1) // R
        mask[m * rows : (m + 1) * rows, :] = jnp.where(rank.astype(f32) == column, 1.0, 0.0)
    dsel[...] = jnp.zeros_like(dsel)
    usel[...] = jnp.zeros_like(usel)
    own_down.wait()
    own_up.wait()
    for d in range(1, tensors):
        landed(dbuf.at[peer(d)], dsem.at[peer(d)])
        landed(ubuf.at[peer(d)], usem.at[peer(d)])
    who = owner[0]
    down, up = dbuf[0], ubuf[0]
    for k in range(1, tensors):
        down = jnp.where(who == k, dbuf[k], down)
        up = jnp.where(who == k, ubuf[k], up)
    dsel[:, 0:ranks] = down
    usel[0:ranks, :] = up
    send_gain.wait_recv()

    def widen(kept):
        return jnp.concatenate([kept, jnp.zeros((kept.shape[0], TILE - ranks), bf16)], axis=1)

    def first(accs):
        own_hidden.wait()
        for d in range(1, tensors):
            landed(x0.at[peer(d)], hidsem.at[peer(d)])
        square = jnp.zeros((tokens, 128), f32)
        for k in range(tensors):
            for hh in range(2):
                def prepare(i, square, k=k, hh=hh):
                    x = x0[k, :, at(hh * piece + i * TILE, TILE)].astype(f32)
                    where_gain = at(k * piece + i * TILE, TILE)
                    g = jnp.where(h == hh, gain[0:1, where_gain].astype(f32), gother[0:1, where_gain].astype(f32))
                    xg0[(2 * k + hh) * tiles + i] = (x * g).astype(bf16)
                    for v in range(TILE // 128):
                        y = x[:, v * 128 : (v + 1) * 128]
                        square = square + y * y
                    return square
                square = lax.fori_loop(0, tiles, prepare, square)
        scale = lax.rsqrt(jnp.sum(square, axis=1, keepdims=True) / full + epsilon)

        steps = []
        for i in range(0, tiles, 2):
            steps.append([
                (
                    lambda i=i, q=q: dsel[(i + q) * TILE : (i + q + 1) * TILE, :],
                    accs[0][q],
                    lambda i=i, q=q: xg0[b * tiles + i + q],
                )
                for q in range(2)
            ])
        run(steps)
        low = pltpu.matmul_pop(accs[0][0]) + pltpu.matmul_pop(accs[0][1])
        lowbuf[b] = low[:, 0:ranks]
        low_sends(0, lowbuf.at[b])

        def main(j):
            def quarter(k, _):
                weight_cols(j, k).wait()
                deep = depth // TILE
                steps = []
                for i in range(deep):
                    steps.append([
                        (
                            lambda i=i, q=q: w[at(k * depth + i * TILE, TILE), j * step + q * TILE : j * step + (q + 1) * TILE],
                            accs[j][q],
                            lambda i=i: xg0[k * deep + i],
                        )
                        for q in range(2)
                    ])
                run(steps)
                return 0
            lax.fori_loop(0, quarters, quarter, 0)

        def finish(j):
            run([[
                (
                    lambda q=q: usel[:, j * step + q * TILE : j * step + (q + 1) * TILE],
                    accs[j][q],
                    lambda: kept0[...],
                )
                for q in range(2)
            ]])
            for q in range(2):
                old = x0[t, :, at(h * piece + j * step + q * TILE, TILE)].astype(f32)
                fresh = (old + pltpu.matmul_pop(accs[j][q]) * scale).astype(bf16)
                for m in range(units):
                    outbuf[m, j, :, q * TILE : (q + 1) * TILE] = fresh[m * rows : (m + 1) * rows]

            @pl.when(jnp.logical_not(last))
            def _():
                for m in range(min(2, units)):
                    send_out(m, j).start()
            for m in range(units):
                write_out(m, j).start()

        early = min(2, chunks)
        for j in range(early):
            main(j)
        for blk in low_blocks():
            landed(lowbuf.at[blk], lsem.at[0, blk])
        low = lowbuf[0]
        for k in range(1, 2 * tensors):
            low = low + lowbuf[k]
        kept0[...] = widen((low * mask[...]).astype(bf16))
        for j in range(early):
            finish(j)
        for j in range(early, chunks):
            main(j)
            finish(j)

        @pl.when(jnp.logical_not(last))
        def _():
            for m in range(2, units):
                for j in range(chunks):
                    send_out(m, j).start()

    arrivals = sorted(
        [(c, 0, c) for c in range(chunks)]
        + [(c + 1.4, 1, c) for c in range(chunks)]
        + [(c + 3.4, 2, c) for c in range(chunks)]
        + [(c + 4.8, 3, c) for c in range(chunks)]
    )

    def later(accs, lows):
        for j in range(chunks):
            for k in range(quarters):
                weight_rows(j, k).wait()

        def unit(m, _):
            here = {"square": jnp.zeros((rows, 128), f32)}
            steps = []

            def pieces(kind):
                hh = h if kind < 2 else 1 - h
                gains = gain if kind < 2 else gother
                if kind % 2 == 0:
                    return [(t, 2 * t + hh, gains)]
                return [(peer(d), 2 * peer(d) + hh, gains) for d in range(1, tensors)]

            def arrive(kind, c, owner_of, blk):
                if kind == 0:
                    landed(xbuf.at[m, blk, c], ysem.at[m, c])
                    remote(xbuf.at[m, blk, c], xbuf.at[m, blk, c], xsend.at[m], xsem.at[m, c], other, t).start()
                elif kind == 2:
                    landed(xbuf.at[m, blk, c], xsem.at[m, c])
                else:
                    landed(xbuf.at[m, blk, c], psem.at[m, owner_of, kind // 2, c])
                if kind % 2 == 0:
                    for d in range(1, tensors):
                        remote(
                            xbuf.at[m, blk, c], xbuf.at[m, blk, c],
                            fsend.at[m], psem.at[m, t, kind // 2, c], s, peer(d),
                        ).start()

            def prepare(c, owner_of, blk, gains):
                x = xbuf[m, blk, c].astype(f32)
                g = gains[0:1, at(owner_of * piece + c * step, step)].astype(f32)
                here["x"] = (x * g).astype(bf16)
                for v in range(step // 128):
                    y = x[:, v * 128 : (v + 1) * 128]
                    here["square"] = here["square"] + y * y

            def lhs(i):
                return lambda: here["x"][:, i * TILE : (i + 1) * TILE]

            def product(blk, c, i, j):
                return [
                    (
                        lambda q=q: w[
                            at(blk * piece + c * step + i * TILE, TILE),
                            j * step + q * TILE : j * step + (q + 1) * TILE,
                        ],
                        accs[j][q],
                        lhs(i),
                    )
                    for q in range(2)
                ]

            def low_product(c, i):
                return [
                    (
                        lambda q=q: dsel[c * step + (i + q) * TILE : c * step + (i + q + 1) * TILE, :],
                        lows[q],
                        lhs(i + q),
                    )
                    for q in range(2)
                ]

            def low_out():
                low = pltpu.matmul_pop(lows[0]) + pltpu.matmul_pop(lows[1])
                lowbuf[b, unit_rows(m), :] = low[:, 0:ranks]
                low_sends(m, lowbuf.at[b, unit_rows(m)])

            def low_in():
                for blk in low_blocks():
                    landed(lowbuf.at[blk, unit_rows(m)], lsem.at[m, blk])
                low = lowbuf[0, unit_rows(m), :]
                for k in range(1, 2 * tensors):
                    low = low + lowbuf[k, unit_rows(m), :]
                here["kept"] = widen((low * mask[unit_rows(m), :]).astype(bf16))

            work = [(kind, c) + p for _, kind, c in arrivals for p in pieces(kind)]
            pending = False
            for kind, c, owner_of, blk, gains in work[:-1]:
                steps.append(lambda a=(kind, c, owner_of, blk): arrive(*a))
                steps.append(lambda a=(c, owner_of, blk, gains): prepare(*a))
                for i in range(inner):
                    for j in range(chunks):
                        steps.append(product(blk, c, i, j))
                if kind == 0:
                    for i in range(0, inner, 2):
                        steps.append(low_product(c, i))
                if pending:
                    steps.append(low_out)
                pending = kind == 0 and c == chunks - 1
            if pending:
                steps.append(low_out)

            kind, c, owner_of, blk, gains = work[-1]
            steps.append(low_in)
            steps.append(lambda: arrive(kind, c, owner_of, blk))
            steps.append(lambda: prepare(c, owner_of, blk, gains))

            def scaling():
                total = jnp.sum(here["square"], axis=1, keepdims=True)
                here["scale"] = lax.rsqrt(total / full + epsilon)

            def leave(j):
                for q in range(2):
                    cols = slice(q * TILE, (q + 1) * TILE)
                    old = xbuf[m, b, j, :, cols].astype(f32)
                    fresh = old + pltpu.matmul_pop(accs[j][q]) * here["scale"]
                    outbuf[m, j, :, cols] = fresh.astype(bf16)

                @pl.when(jnp.logical_not(last))
                def _():
                    send_out(m, j).start()
                write_out(m, j).start()

            for j in range(chunks):
                for i in range(inner):
                    steps.append(product(blk, c, i, j))
                steps.append([
                    (
                        lambda j=j, q=q: usel[:, j * step + q * TILE : j * step + (q + 1) * TILE],
                        accs[j][q],
                        lambda: here["kept"],
                    )
                    for q in range(2)
                ])
                if j == 0:
                    steps.append(scaling)
                if j > 0:
                    steps.append(lambda j=j: leave(j - 1))
            steps.append(lambda: leave(chunks - 1))
            run(steps)
            return 0

        lax.fori_loop(0, units, unit, 0)

        for m in range(units):
            landed(xbuf.at[m, 0], xsend.at[m])
            if tensors > 1:
                landed(xbuf.at[m, 0 : 2 * (tensors - 1)], fsend.at[m])
            landed(lowbuf.at[0 : 2 * tensors - 1, m * rows : (m + 1) * rows], lsend.at[m])

    def body(*flat):
        for acc in flat:
            pltpu.matmul_pop(acc)
        wide = [flat[2 * j : 2 * j + 2] for j in range(chunks)]
        narrow = [flat[2 * (chunks + j) : 2 * (chunks + j) + 2] for j in range(chunks)]
        lows = flat[4 * chunks :]

        @pl.when(level == 0)
        def _():
            first(wide)

        @pl.when(level > 0)
        def _():
            later(narrow, lows)

    def acc(q, height):
        return pltpu.ACC(q)((height, TILE), f32)

    pl.run_scoped(
        body,
        *[acc(q, tokens) for _ in range(chunks) for q in range(2)],
        *[acc(q, rows) for _ in range(chunks) for q in range(2)],
        *[acc(q, rows) for q in range(2)],
    )

    send_gain.wait_send()
    for d in range(1, tensors):
        send_down(d).wait_send()
        send_up(d).wait_send()

    @pl.when(level == 0)
    def _():
        for d in range(1, tensors):
            send_hidden(d).wait_send()
        landed(lowbuf.at[0 : 2 * tensors - 1], lsend.at[0])

    @pl.when(jnp.logical_not(last))
    def _():
        for m in range(units):
            landed(outbuf.at[m], osend.at[m])

    for m in range(units):
        landed(outbuf.at[m], wout.at[m])


def local(
    hidden_in, segment_ids, segment_job, job_adapter, owner, frozen, norm_gain, inbox_down, inbox_up
):
    tensors = lax.axis_size("tensor")
    sections = lax.axis_size("section")
    units, rows = segment_ids.shape
    depth, piece = frozen.shape[1:]
    ranks = inbox_down.shape[3]
    step = 2 * TILE
    chunks = piece // step
    quarters = 4
    tokens = units * rows
    anywhere = pl.BlockSpec(memory_space=pl.ANY)
    smem = pl.BlockSpec(memory_space=pltpu.SMEM)
    vmem = pl.BlockSpec(memory_space=pltpu.VMEM)
    dma = pltpu.SemaphoreType.DMA
    body = functools.partial(
        kernel, sections, tensors, units, rows, piece, chunks, quarters, ranks,
        (segment_job.shape[1], job_adapter.shape[0]),
    )
    return pl.pallas_call(
        body,
        out_shape=jax.ShapeDtypeStruct((1, tokens, piece), bf16),
        in_specs=[anywhere, vmem, smem, smem, smem, anywhere, vmem, anywhere, anywhere],
        out_specs=anywhere,
        scratch_shapes=[
            pltpu.VMEM((depth, piece), bf16),
            pltpu.VMEM((tensors, tokens, 2 * piece), bf16),
            pltpu.VMEM((depth // TILE, tokens, TILE), bf16),
            pltpu.VMEM((units, 2 * tensors, chunks, rows, step), bf16),
            pltpu.VMEM((units, chunks, rows, step), bf16),
            pltpu.VMEM(norm_gain.shape, bf16),
            pltpu.VMEM((tensors, piece, ranks), bf16),
            pltpu.VMEM((tensors, ranks, piece), bf16),
            pltpu.VMEM((piece, TILE), bf16),
            pltpu.VMEM((TILE, piece), bf16),
            pltpu.VMEM((2 * tensors, tokens, ranks), f32),
            pltpu.VMEM((tokens, ranks), f32),
            pltpu.VMEM((tokens, TILE), bf16),
            dma((chunks, quarters)),
            dma((tensors,)),
            dma((tensors,)),
            dma((tensors,)),
            dma((tensors,)),
            dma((2, tensors)),
            dma((2,)),
            dma((units, chunks)),
            dma((units, chunks)),
            dma((units, tensors, 2, chunks)),
            dma((units, 2 * tensors)),
            dma((units,)),
            dma((units,)),
            dma((units,)),
            dma((units,)),
            dma((units,)),
        ],
        compiler_params=pltpu.CompilerParams(
            collective_id=0, has_side_effects=True, vmem_limit_bytes=60 * 2**20
        ),
    )(hidden_in, segment_ids, segment_job, job_adapter, owner, frozen, norm_gain, inbox_down, inbox_up)


def solution(mesh):
    mapped = jax.shard_map(
        local,
        mesh=mesh,
        in_specs=(
            P(None, "tensor"),
            P(),
            P(),
            P(),
            P("section"),
            P("section", None, "tensor"),
            P("section", None),
            P("section", "tensor", None, None),
            P("section", "tensor", None, None),
        ),
        out_specs=P("section", None, "tensor"),
        check_vma=False,
    )
    return mapped
```

```python
import functools
import jax
import jax.numpy as jnp
from jax import lax
from jax.experimental import pallas as pl
from jax.experimental.pallas import tpu as pltpu
from jax.sharding import PartitionSpec as P

R = 32
TILE = 256
UNIT = 32
DIRECT = 0
EARLY = 0
TAIL = 2
LAG = 4
MESH = pl.DeviceIdType.MESH
epsilon = 1e-05
f32, bf16 = jnp.float32, jnp.bfloat16


def products_of(steps):
    return [step for step in steps if isinstance(step, list)]


def stage(product, n):
    for q, (rhs, _, _) in enumerate(product):
        pltpu.matmul_push_rhs(rhs(), staging_register=n % 2, mxu_index=q)


def run(steps, carried=False):
    products = products_of(steps)
    count = len(products)
    if not carried:
        for n in range(min(2, count)):
            stage(products[n], n)
    n = 0
    for step in steps:
        if isinstance(step, list):
            for _, acc, lhs in step:
                pltpu.matmul_acc_lhs(acc, lhs(), load_staged_rhs=n % 2)
            if n + 2 < count:
                stage(products[n + 2], n)
            elif carried:
                stage(products[n + 2 - count], n)
            n += 1
        else:
            with jax.named_scope(getattr(step, "label", "step")):
                step()


def kernel(
    sections, tensors, batches, rows, piece, chunks, ranks, jobs_of,
    hidden, ids, seg_job, job_ad, owner, frozen, gain, idown, iup,
    out,
    w, x0, xg0, xbuf, outbuf, gother, dout, uout, dbuf, ubuf, dsel, usel, lowbuf, mask, kept0, sq0,
    wsem, hidsem, hidsend, ready, dsem, usem, isend, gsem, ysem, xsem, psem, lsem,
    osend, xsend, fsend, lsend, wout,
):
    levels = sections // 2
    step = piece // chunks
    batch, spread = batches
    tokens = batch * spread
    units = -(-tokens // rows)
    short = tokens - (units - 1) * rows
    full = 2 * tensors * piece
    blocks = 2 * tensors
    inner = step // TILE
    tiles = piece // TILE
    segs, jobs = jobs_of
    window = 6
    direct = min(DIRECT, chunks - 1)
    early = min(EARLY, chunks - 1)
    s = lax.axis_index("section")
    t = lax.axis_index("tensor")
    h = lax.rem(s, 2)
    level = s // 2
    other = s + 1 - 2 * h
    b = 2 * t + h
    last = level == levels - 1

    def peer(d):
        return lax.rem(t + d, tensors)

    def at(start, size):
        return pl.ds(pl.multiple_of(start, TILE), size)

    def part(k):
        return at(k * piece, piece)

    def remote(src, dst, send, recv, section, tensor):
        return pltpu.make_async_remote_copy(
            src_ref=src, dst_ref=dst, send_sem=send, recv_sem=recv,
            device_id=(section, tensor), device_id_type=MESH,
        )

    def landed(ref, sem):
        pltpu.make_async_copy(ref, ref, sem).wait()

    def unit_rows(m):
        return pl.ds(pl.multiple_of(m * rows, 8), rows)

    own_hidden = pltpu.make_async_copy(hidden, x0.at[t], hidsem.at[t])
    own_down = pltpu.make_async_copy(idown.at[0, 0, part(t), :], dbuf.at[t], dsem.at[t])
    own_up = pltpu.make_async_copy(iup.at[0, 0, :, part(t)], ubuf.at[t], usem.at[t])

    def read_down(d):
        return pltpu.make_async_copy(idown.at[0, 0, part(peer(d)), :], dout.at[d], ready.at[0, d])

    def read_up(d):
        return pltpu.make_async_copy(iup.at[0, 0, :, part(peer(d))], uout.at[d], ready.at[1, d])

    def weight_cols(j, blk):
        here = (part(blk), at(j * step, step))
        return pltpu.make_async_copy(frozen.at[(0,) + here], w.at[here], wsem.at[j, blk])

    def weight_rows(j, blk):
        here = at(blk * piece + j * step, step)
        return pltpu.make_async_copy(frozen.at[0, here, :], w.at[here, :], wsem.at[j, blk])

    def rest():
        return [2 * t + 1 - h] + [2 * peer(d) + hh for d in range(1, tensors) for hh in range(2)]

    barrier = pltpu.get_barrier_semaphore()

    def greet(section, tensor):
        pl.semaphore_signal(barrier, inc=1, device_id=(section, tensor), device_id_type=MESH)

    for d in range(1, tensors):
        greet(s, peer(d))
    for d in range(tensors):
        greet(other, peer(d))

    @pl.when(level > 0)
    def _():
        greet(s - 2, t)
        greet(other - 2, t)

    @pl.when(level < levels - 1)
    def _():
        greet(s + 2, t)
        greet(other + 2, t)

    @pl.when(level == 0)
    def _():
        own_hidden.start()

    def read_adapters():
        own_down.start()
        own_up.start()

    for d in range(1, tensors):
        read_down(d).start()
        read_up(d).start()

    fetches = [(j, b) for j in range(chunks)] + [(j, blk) for j in range(chunks) for blk in rest()]

    def fetch(n):
        if n < len(fetches):
            weight_cols(*fetches[n]).start()

    def fetched(n):
        weight_cols(*fetches[n]).wait()
        fetch(n + window)

    @pl.when(level == 0)
    def _():
        fetch(0)

    @pl.when(level > 0)
    def _():
        read_adapters()
        for j in range(chunks):
            for blk in range(blocks):
                weight_rows(j, blk).start()

    def gain_row(hh, start, size):
        near = gain[0:1, at(start, size)].astype(f32)
        return near if hh is None else jnp.where(h == hh, near, gother[0:1, at(start, size)].astype(f32))

    def prepare_first(owner_of, hh, square):
        blk = 2 * owner_of + (h if hh is None else hh)
        start = (h if hh is None else hh) * piece

        def one(i, square):
            x = x0[owner_of, :, at(start + i * TILE, TILE)].astype(f32)
            xg0[blk * tiles + i] = (x * gain_row(hh, owner_of * piece + i * TILE, TILE)).astype(bf16)
            for v in range(TILE // 128):
                y = x[:, v * 128 : (v + 1) * 128]
                square = square + y * y
            return square

        return lax.fori_loop(0, tiles, one, square)

    @pl.when(level == 0)
    def _():
        own_hidden.wait()
        for n in range(1, 3):
            fetch(n)
        read_adapters()
        for n in range(3, window):
            fetch(n)
        sq0[...] = prepare_first(t, None, jnp.zeros((tokens, 128), f32))

    ends = (level > 0).astype(jnp.int32) + (level < levels - 1).astype(jnp.int32)
    with jax.named_scope("barrier"):
        pl.semaphore_wait(barrier, 2 * tensors - 1 + 2 * ends)

    def send_hidden(d):
        return remote(x0.at[t], x0.at[t], hidsend.at[d], hidsem.at[t], s, peer(d))

    def send_down(d):
        return remote(dout.at[d], dbuf.at[t], isend.at[0, d], dsem.at[t], s, peer(d))

    def send_up(d):
        return remote(uout.at[d], ubuf.at[t], isend.at[1, d], usem.at[t], s, peer(d))

    send_gain = remote(gain, gother, gsem.at[0], gsem.at[1], other, t)
    send_gain.start()

    @pl.when(level == 0)
    def _():
        for d in range(1, tensors):
            send_hidden(d).start()

    for d in range(1, tensors):
        read_down(d).wait()
        send_down(d).start()
        read_up(d).wait()
        send_up(d).start()

    def send_out(m, c):
        return remote(outbuf.at[m, c], xbuf.at[m, b, c], osend.at[m], ysem.at[m, c], s + 2, t)

    def send_across(m, c):
        return remote(outbuf.at[m, c], xbuf.at[m, b, c], osend.at[m], xsem.at[m, c], other + 2, t)

    def send_both(m, c):
        send_out(m, c).start()
        if c >= chunks - direct:
            send_across(m, c).start()

    def sent(m):
        landed(outbuf.at[m], osend.at[m])
        if direct:
            landed(outbuf.at[m, 0:direct], osend.at[m])

    def write_out(m, c):
        def write(size):
            here = pl.ds(pl.multiple_of(m * rows, 8), size)
            pltpu.make_async_copy(
                outbuf.at[m, c, 0:size], out.at[0, here, at(c * step, step)], wout.at[m]
            ).start()

        if short == rows:
            write(rows)
        elif isinstance(m, int):
            write(short if m == units - 1 else rows)
        else:
            pl.when(m < units - 1)(lambda: write(rows))
            pl.when(m == units - 1)(lambda: write(short))

    def low_sends(slot, ref):
        for side in range(2):
            for d in range(1 - side, tensors):
                remote(ref, ref, lsend.at[slot], lsem.at[slot, b], s if side == 0 else other, peer(d)).start()

    def low_blocks():
        return [2 * peer(d) + (h if side == 0 else 1 - h) for side in range(2) for d in range(1 - side, tensors)]

    for m in range(batch):
        seg = ids[pl.ds(m, 1), :]
        slot = jnp.zeros_like(seg)
        for g in range(segs):
            slot = jnp.where(seg == g, job_ad[seg_job[m, g]], slot)
        square_of = (spread, spread)
        eye = lax.broadcasted_iota(jnp.int32, square_of, 0) == lax.broadcasted_iota(jnp.int32, square_of, 1)
        lanes = jnp.where(eye, jnp.broadcast_to(slot.astype(f32), square_of), 0.0)
        column = jnp.sum(lanes, axis=1, keepdims=True)
        rank = lax.broadcasted_iota(jnp.int32, (spread, ranks), 1) // R
        mask[m * spread : (m + 1) * spread, :] = jnp.where(rank.astype(f32) == column, 1.0, 0.0)
    if short < rows:
        mask[tokens:, :] = jnp.zeros((units * rows - tokens, ranks), f32)

    def adapters():
        own_down.wait()
        own_up.wait()
        for d in range(1, tensors):
            landed(dbuf.at[peer(d)], dsem.at[peer(d)])
            landed(ubuf.at[peer(d)], usem.at[peer(d)])
        who = owner[0]
        down, up = dbuf[0], ubuf[0]
        for k in range(1, tensors):
            down = jnp.where(who == k, dbuf[k], down)
            up = jnp.where(who == k, ubuf[k], up)
        dsel[:, 0:ranks] = down
        dsel[:, ranks:] = jnp.zeros((piece, TILE - ranks), bf16)
        usel[0:ranks, :] = up
        usel[ranks:, :] = jnp.zeros((TILE - ranks, piece), bf16)

    def widen(kept):
        return jnp.concatenate([kept, jnp.zeros((kept.shape[0], TILE - ranks), kept.dtype)], axis=1)

    def first(accs, lows):
        def main(j, begin, end):
            steps = []
            for n, (_, blk) in enumerate(fetches[begin:end]):
                wait = lambda n=n: fetched(begin + n)
                wait.label = "wwait"
                if n == 0:
                    wait()
                else:
                    steps.insert(n * tiles - 2 + n - 1, wait)
                for i in range(tiles):
                    steps.append([
                        (
                            lambda i=i, q=q, blk=blk: w[
                                at(blk * piece + i * TILE, TILE), j * step + q * TILE : j * step + (q + 1) * TILE
                            ],
                            accs[j][q],
                            lambda i=i, blk=blk: xg0[blk * tiles + i],
                        )
                        for q in range(2)
                    ])
            run(steps)

        for j in range(chunks):
            main(j, j, j + 1)
        with jax.named_scope("gainwait"):
            send_gain.wait_recv()
        square = prepare_first(t, 1 - h, sq0[...])
        for d in range(1, tensors):
            with jax.named_scope("hidwait"):
                landed(x0.at[peer(d)], hidsem.at[peer(d)])
            for hh in range(2):
                square = prepare_first(peer(d), hh, square)
        scale = lax.rsqrt(jnp.sum(square, axis=1, keepdims=True) / full + epsilon)

        with jax.named_scope("adapters"):
            adapters()
        steps = []
        for i in range(0, tiles, 2):
            steps.append([
                (
                    lambda i=i, q=q: dsel[(i + q) * TILE : (i + q + 1) * TILE, :],
                    lows[q],
                    lambda i=i, q=q: xg0[b * tiles + i + q],
                )
                for q in range(2)
            ])
        run(steps)
        low = pltpu.matmul_pop(lows[0]) + pltpu.matmul_pop(lows[1])
        lowbuf[b, 0:tokens] = low[:, 0:ranks]
        low_sends(0, lowbuf.at[b, 0:tokens])

        def finish(j):
            run([[
                (
                    lambda q=q: usel[:, j * step + q * TILE : j * step + (q + 1) * TILE],
                    accs[j][q],
                    lambda: kept0[...],
                )
                for q in range(2)
            ]])
            for q in range(2):
              with jax.named_scope('fin'):
                old = x0[t, :, at(h * piece + j * step + q * TILE, TILE)].astype(f32)
                fresh = old + pltpu.matmul_pop(accs[j][q]) * scale
                for m in range(units):
                    size = short if m == units - 1 else rows
                    cols = slice(q * TILE, (q + 1) * TILE)
                    outbuf[m, j, 0:size, cols] = fresh[m * rows : m * rows + size].astype(bf16)
                    if size < rows:
                        outbuf[m, j, size:, cols] = jnp.zeros((rows - size, TILE), bf16)

            @pl.when(jnp.logical_not(last))
            def _():
                send_both(0, j)
            for m in range(units):
                write_out(m, j)

        ready_chunks = min(2, chunks)
        for j in range(ready_chunks):
            main(j, chunks + j * len(rest()), chunks + (j + 1) * len(rest()))
        with jax.named_scope("lowwait"):
            for blk in low_blocks():
                landed(lowbuf.at[blk, 0:tokens], lsem.at[0, blk])
        low = lowbuf[0, 0:tokens]
        for k in range(1, 2 * tensors):
            low = low + lowbuf[k, 0:tokens]
        kept0[...] = widen((low * mask[0:tokens]).astype(bf16))
        for j in range(ready_chunks):
            finish(j)
        for j in range(ready_chunks, chunks):
            main(j, chunks + j * len(rest()), chunks + (j + 1) * len(rest()))
            finish(j)

        @pl.when(jnp.logical_not(last))
        def _():
            for m in range(1, units):
                sent(m - 1)
                for j in range(chunks):
                    send_both(m, j)
            sent(units - 1)

    crossing = list(range(chunks - direct, chunks))
    relayed = list(range(chunks - direct))
    arrivals = [(0, kind, c) for kind in range(2) for c in range(chunks)]
    late = relayed[:1] + crossing + relayed[1:]
    arrivals += [(0, kind, c) for kind in range(2, 4) for c in late]
    lead = min(3, inner * chunks - 1)

    def label(name, step):
        step.label = name
        return step

    def later(accs, lows):
        adapters()
        send_gain.wait_recv()
        with jax.named_scope("wrow"):
            for j in range(chunks):
                for blk in range(blocks):
                    weight_rows(j, blk).wait()

        def pieces(kind):
            hh = h if kind < 2 else 1 - h
            gains = gain if kind < 2 else gother
            if kind % 2 == 0:
                return [(t, 2 * t + hh, gains)]
            return [(peer(d), 2 * peer(d) + hh, gains) for d in range(1, tensors)]

        work = [(kind, c) + p for _, kind, c in arrivals for p in pieces(kind)]

        def arrive(m, kind, c, owner_of, blk):
            ref = xbuf.at[m, blk, c]
            if kind == 0:
                landed(ref, ysem.at[m, c])
                if c < chunks - direct:
                    remote(ref, ref, xsend.at[m], xsem.at[m, c], other, t).start()
            elif kind == 2:
                landed(ref, xsem.at[m, c])
            else:
                landed(ref, psem.at[m, owner_of, kind // 2, c])
            if kind % 2 == 0:
                for d in range(1, tensors):
                    remote(ref, ref, fsend.at[m], psem.at[m, t, kind // 2, c], s, peer(d)).start()

        def unit_steps(m):
            here = {"square": jnp.zeros((rows, 128), f32)}
            steps = []

            def prepare(key):
                _, c, owner_of, blk, gains = work[key]
                x = xbuf[m, blk, c].astype(f32)
                here[key] = x * gains[0:1, at(owner_of * piece + c * step, step)].astype(f32)
                for v in range(step // 128):
                    y = x[:, v * 128 : (v + 1) * 128]
                    here["square"] = here["square"] + y * y

            def lhs(key, i):
                return lambda: here[key][:, i * TILE : (i + 1) * TILE]

            def product(key, i, j):
                _, c, _, blk, _ = work[key]
                return [
                    (
                        lambda q=q: w[
                            at(blk * piece + c * step + i * TILE, TILE),
                            j * step + q * TILE : j * step + (q + 1) * TILE,
                        ],
                        accs[j][q],
                        lhs(key, i),
                    )
                    for q in range(2)
                ]

            def low_product(key, i):
                start = work[key][1] * step + i * TILE
                return [
                    (
                        lambda q=q: dsel[start + q * TILE : start + (q + 1) * TILE, :],
                        lows[q],
                        lhs(key, i + q),
                    )
                    for q in range(2)
                ]

            def low_out():
                low = pltpu.matmul_pop(lows[0]) + pltpu.matmul_pop(lows[1])
                lowbuf[b, unit_rows(m), :] = low[:, 0:ranks]
                low_sends(m, lowbuf.at[b, unit_rows(m)])

            def low_in():
                for blk in low_blocks():
                    landed(lowbuf.at[blk, unit_rows(m)], lsem.at[m, blk])
                low = lowbuf[0, unit_rows(m), :]
                for k in range(1, 2 * tensors):
                    low = low + lowbuf[k, unit_rows(m), :]
                here["kept"] = widen(low * mask[unit_rows(m), :])

            def meet(key):
                kind, c, owner_of, blk, _ = work[key]
                found = [lambda: prepare(key)]
                if kind > 0 or c >= early:
                    name = "arr" + "YDXE"[kind] + str(c)
                    found = [label(name, lambda: arrive(m, kind, c, owner_of, blk))] + found
                return found

            def scaling():
                total = jnp.sum(here["square"], axis=1, keepdims=True)
                here["scale"] = lax.rsqrt(total / full + epsilon)

            def leave(j):
                for q in range(2):
                    cols = slice(q * TILE, (q + 1) * TILE)
                    old = xbuf[m, b, j, :, cols].astype(f32)
                    fresh = old + pltpu.matmul_pop(accs[j][q]) * here["scale"]
                    outbuf[m, j, :, cols] = fresh.astype(bf16)

                @pl.when(jnp.logical_not(last))
                def _():
                    send_both(m, j)
                write_out(m, j)
                if j < early:
                    @pl.when(m + 1 < units)
                    def _():
                        arrive(m + 1, 0, j, t, b)

            pending = False
            steps += meet(0)
            tail = len(work) - TAIL
            for key, (kind, c, _, _, _) in enumerate(work[:tail]):
                low_out_at = len(steps) + inner * chunks // 2
                for i in range(inner):
                    for j in range(chunks):
                        steps.append(product(key, i, j))
                if kind == 0:
                    for i in range(0, inner, 2):
                        steps.append(low_product(key, i))
                if pending:
                    steps.insert(low_out_at, label("lowout", low_out))
                pending = kind == 0 and c == chunks - 1
                ahead = meet(key + 1)
                if key + 1 == tail:
                    ahead = [label("lowin", low_in)] + ahead
                    for more in range(tail + 1, len(work)):
                        ahead += meet(more)
                steps[len(steps) - lead : len(steps) - lead] = ahead
            if pending:
                steps.append(low_out)
            for j in range(chunks):
                for key in range(tail, len(work)):
                    for i in range(inner):
                        steps.append(product(key, i, j))
                steps.append([
                    (
                        lambda j=j, q=q: usel[:, j * step + q * TILE : j * step + (q + 1) * TILE],
                        accs[j][q],
                        lambda: here["kept"],
                    )
                    for q in range(2)
                ])
                if j == 0:
                    steps.append(scaling)
                if j > 0:
                    back = len(steps) - max(0, len(products_of(steps[-TAIL * inner - 1 :])) - LAG)
                    steps.insert(back, label("leave", lambda j=j: leave(j - 1)))
            steps.append(label("leave", lambda: leave(chunks - 1)))
            return steps

        begin = products_of(unit_steps(0))
        carried = len(begin) % 2 == 0
        if carried:
            for n in range(2):
                stage(begin[n], n)
        for c in range(early):
            with jax.named_scope("first"):
                arrive(0, 0, c, t, b)

        def unit(m, _):
            run(unit_steps(m), carried)
            return 0

        lax.fori_loop(0, units, unit, 0)
        if carried:
            for n in range(2):
                for q in range(2):
                    pltpu.matmul_acc_lhs(accs[0][q], jnp.zeros((rows, TILE), f32), load_staged_rhs=n)
            for q in range(2):
                pltpu.matmul_pop(accs[0][q])

        for m in range(units):
            if chunks > direct:
                landed(xbuf.at[m, 0, 0 : chunks - direct], xsend.at[m])
            if tensors > 1:
                landed(xbuf.at[m, 0 : 2 * (tensors - 1)], fsend.at[m])
            landed(lowbuf.at[0 : 2 * tensors - 1, m * rows : (m + 1) * rows], lsend.at[m])

    def body(*flat):
        for acc in flat:
            pltpu.matmul_pop(acc)
        pairs = [flat[2 * j : 2 * j + 2] for j in range(2 * chunks + 2)]

        @pl.when(level == 0)
        def _():
            first(pairs[:chunks], pairs[-2])

        @pl.when(level > 0)
        def _():
            later(pairs[chunks:-2], pairs[-1])

    heights = chunks * [tokens] + chunks * [rows] + [tokens, rows]
    pl.run_scoped(body, *[pltpu.ACC(q)((height, TILE), f32) for height in heights for q in range(2)])

    send_gain.wait_send()
    for d in range(1, tensors):
        send_down(d).wait_send()
        send_up(d).wait_send()

    @pl.when(level == 0)
    def _():
        for d in range(1, tensors):
            send_hidden(d).wait_send()
        landed(lowbuf.at[0 : 2 * tensors - 1, 0:tokens], lsend.at[0])

    @pl.when(jnp.logical_not(last) & (level > 0))
    def _():
        for m in range(units):
            sent(m)

    for m in range(units):
        landed(outbuf.at[m, :, 0 : short if m == units - 1 else rows], wout.at[m])


def local(
    hidden_in, segment_ids, segment_job, job_adapter, owner, frozen, norm_gain, inbox_down, inbox_up
):
    tensors = lax.axis_size("tensor")
    sections = lax.axis_size("section")
    batches = segment_ids.shape
    depth, piece = frozen.shape[1:]
    ranks = inbox_down.shape[3]
    step = 2 * TILE
    chunks = piece // step
    tokens = batches[0] * batches[1]
    rows = min(UNIT, tokens)
    units = -(-tokens // rows)
    anywhere = pl.BlockSpec(memory_space=pl.ANY)
    smem = pl.BlockSpec(memory_space=pltpu.SMEM)
    vmem = pl.BlockSpec(memory_space=pltpu.VMEM)
    dma = pltpu.SemaphoreType.DMA
    body = functools.partial(
        kernel, sections, tensors, batches, rows, piece, chunks, ranks,
        (segment_job.shape[1], job_adapter.shape[0]),
    )
    return pl.pallas_call(
        body,
        out_shape=jax.ShapeDtypeStruct((1, tokens, piece), bf16),
        in_specs=[anywhere, vmem, smem, smem, smem, anywhere, vmem, anywhere, anywhere],
        out_specs=anywhere,
        scratch_shapes=[
            pltpu.VMEM((depth, piece), bf16),
            pltpu.VMEM((tensors, tokens, 2 * piece), bf16),
            pltpu.VMEM((depth // TILE, tokens, TILE), bf16),
            pltpu.VMEM((units, 2 * tensors, chunks, rows, step), bf16),
            pltpu.VMEM((units, chunks, rows, step), bf16),
            pltpu.VMEM(norm_gain.shape, bf16),
            pltpu.VMEM((tensors, piece, ranks), bf16),
            pltpu.VMEM((tensors, ranks, piece), bf16),
            pltpu.VMEM((tensors, piece, ranks), bf16),
            pltpu.VMEM((tensors, ranks, piece), bf16),
            pltpu.VMEM((piece, TILE), bf16),
            pltpu.VMEM((TILE, piece), bf16),
            pltpu.VMEM((2 * tensors, units * rows, ranks), f32),
            pltpu.VMEM((units * rows, ranks), f32),
            pltpu.VMEM((tokens, TILE), bf16),
            pltpu.VMEM((tokens, 128), f32),
            dma((chunks, 2 * tensors)),
            dma((tensors,)),
            dma((tensors,)),
            dma((2, tensors)),
            dma((tensors,)),
            dma((tensors,)),
            dma((2, tensors)),
            dma((2,)),
            dma((units, chunks)),
            dma((units, chunks)),
            dma((units, tensors, 2, chunks)),
            dma((units, 2 * tensors)),
            dma((units,)),
            dma((units,)),
            dma((units,)),
            dma((units,)),
            dma((units,)),
        ],
        compiler_params=pltpu.CompilerParams(
            collective_id=0, has_side_effects=True, vmem_limit_bytes=60 * 2**20
        ),
    )(hidden_in, segment_ids, segment_job, job_adapter, owner, frozen, norm_gain, inbox_down, inbox_up)


def solution(mesh):
    mapped = jax.shard_map(
        local,
        mesh=mesh,
        in_specs=(
            P(None, "tensor"),
            P(),
            P(),
            P(),
            P("section"),
            P("section", None, "tensor"),
            P("section", None),
            P("section", "tensor", None, None),
            P("section", "tensor", None, None),
        ),
        out_specs=P("section", None, "tensor"),
        check_vma=False,
    )
    return mapped
```

```python
import functools
import jax
import jax.numpy as jnp
from jax import lax
from jax.experimental import pallas as pl
from jax.experimental.pallas import tpu as pltpu
from jax.sharding import PartitionSpec as P

R = 32
TILE = 256
UNIT = 32
DIRECT = 0
EARLY = 0
DELAYS = (0, 4, 8, 12)
TAIL = 1
LAG = 4
MESH = pl.DeviceIdType.MESH
epsilon = 1e-05
f32, bf16 = jnp.float32, jnp.bfloat16


def products_of(steps):
    return [step for step in steps if isinstance(step, list)]


def stage(product, n):
    for q, (rhs, _, _) in enumerate(product):
        pltpu.matmul_push_rhs(rhs(), staging_register=n % 2, mxu_index=q)


def run(steps, carried=False):
    products = products_of(steps)
    count = len(products)
    if not carried:
        for n in range(min(2, count)):
            stage(products[n], n)
    n = 0
    for step in steps:
        if isinstance(step, list):
            for _, acc, lhs in step:
                pltpu.matmul_acc_lhs(acc, lhs(), load_staged_rhs=n % 2)
            if n + 2 < count:
                stage(products[n + 2], n)
            elif carried:
                stage(products[n + 2 - count], n)
            n += 1
        else:
            with jax.named_scope(getattr(step, "label", "step")):
                step()


def kernel(
    sections, tensors, batches, rows, piece, chunks, ranks, jobs_of,
    hidden, ids, seg_job, job_ad, owner, frozen, gain, idown, iup,
    out,
    w, x0, xg0, xbuf, outbuf, gother, dout, uout, dbuf, ubuf, dsel, usel, lowbuf, mask, kept0, sq0,
    wsem, hidsem, hidsend, ready, dsem, usem, isend, gsem, ysem, xsem, psem, lsem,
    osend, xsend, fsend, lsend, wout,
):
    levels = sections // 2
    step = piece // chunks
    batch, spread = batches
    tokens = batch * spread
    units = -(-tokens // rows)
    short = tokens - (units - 1) * rows
    full = 2 * tensors * piece
    blocks = 2 * tensors
    inner = step // TILE
    tiles = piece // TILE
    segs, jobs = jobs_of
    window = 6
    direct = min(DIRECT, chunks - 1)
    early = min(EARLY, chunks - 1)
    s = lax.axis_index("section")
    t = lax.axis_index("tensor")
    h = lax.rem(s, 2)
    level = s // 2
    other = s + 1 - 2 * h
    b = 2 * t + h
    last = level == levels - 1

    def peer(d):
        return lax.rem(t + d, tensors)

    def at(start, size):
        return pl.ds(pl.multiple_of(start, TILE), size)

    def part(k):
        return at(k * piece, piece)

    def remote(src, dst, send, recv, section, tensor):
        return pltpu.make_async_remote_copy(
            src_ref=src, dst_ref=dst, send_sem=send, recv_sem=recv,
            device_id=(section, tensor), device_id_type=MESH,
        )

    def landed(ref, sem):
        pltpu.make_async_copy(ref, ref, sem).wait()

    def unit_rows(m):
        return pl.ds(pl.multiple_of(m * rows, 8), rows)

    own_hidden = pltpu.make_async_copy(hidden, x0.at[t], hidsem.at[t])
    own_down = pltpu.make_async_copy(idown.at[0, 0, part(t), :], dbuf.at[t], dsem.at[t])
    own_up = pltpu.make_async_copy(iup.at[0, 0, :, part(t)], ubuf.at[t], usem.at[t])

    def read_down(d):
        return pltpu.make_async_copy(idown.at[0, 0, part(peer(d)), :], dout.at[d], ready.at[0, d])

    def read_up(d):
        return pltpu.make_async_copy(iup.at[0, 0, :, part(peer(d))], uout.at[d], ready.at[1, d])

    def weight_cols(j, blk):
        here = (part(blk), at(j * step, step))
        return pltpu.make_async_copy(frozen.at[(0,) + here], w.at[here], wsem.at[j, blk])

    def weight_rows(j, blk):
        here = at(blk * piece + j * step, step)
        return pltpu.make_async_copy(frozen.at[0, here, :], w.at[here, :], wsem.at[j, blk])

    def rest():
        return [2 * t + 1 - h] + [2 * peer(d) + hh for d in range(1, tensors) for hh in range(2)]

    barrier = pltpu.get_barrier_semaphore()

    def greet(section, tensor):
        pl.semaphore_signal(barrier, inc=1, device_id=(section, tensor), device_id_type=MESH)

    for d in range(1, tensors):
        greet(s, peer(d))
    for d in range(tensors):
        greet(other, peer(d))

    @pl.when(level > 0)
    def _():
        greet(s - 2, t)
        greet(other - 2, t)

    @pl.when(level < levels - 1)
    def _():
        greet(s + 2, t)
        greet(other + 2, t)

    @pl.when(level == 0)
    def _():
        own_hidden.start()

    def read_adapters():
        own_down.start()
        own_up.start()

    for d in range(1, tensors):
        read_down(d).start()
        read_up(d).start()

    fetches = [(j, b) for j in range(chunks)] + [(j, blk) for j in range(chunks) for blk in rest()]

    def fetch(n):
        if n < len(fetches):
            weight_cols(*fetches[n]).start()

    def fetched(n):
        weight_cols(*fetches[n]).wait()
        fetch(n + window)

    @pl.when(level == 0)
    def _():
        fetch(0)

    @pl.when(level > 0)
    def _():
        read_adapters()
        for j in range(chunks):
            for blk in range(blocks):
                weight_rows(j, blk).start()

    def gain_row(hh, start, size):
        near = gain[0:1, at(start, size)].astype(f32)
        return near if hh is None else jnp.where(h == hh, near, gother[0:1, at(start, size)].astype(f32))

    def prepare_first(owner_of, hh, square):
        blk = 2 * owner_of + (h if hh is None else hh)
        start = (h if hh is None else hh) * piece

        def one(i, square):
            x = x0[owner_of, :, at(start + i * TILE, TILE)].astype(f32)
            xg0[blk * tiles + i] = (x * gain_row(hh, owner_of * piece + i * TILE, TILE)).astype(bf16)
            for v in range(TILE // 128):
                y = x[:, v * 128 : (v + 1) * 128]
                square = square + y * y
            return square

        return lax.fori_loop(0, tiles, one, square)

    @pl.when(level == 0)
    def _():
        own_hidden.wait()
        for n in range(1, 3):
            fetch(n)
        read_adapters()
        for n in range(3, window):
            fetch(n)
        sq0[...] = prepare_first(t, None, jnp.zeros((tokens, 128), f32))

    ends = (level > 0).astype(jnp.int32) + (level < levels - 1).astype(jnp.int32)
    with jax.named_scope("barrier"):
        pl.semaphore_wait(barrier, 2 * tensors - 1 + 2 * ends)

    def send_hidden(d):
        return remote(x0.at[t], x0.at[t], hidsend.at[d], hidsem.at[t], s, peer(d))

    def send_down(d):
        return remote(dout.at[d], dbuf.at[t], isend.at[0, d], dsem.at[t], s, peer(d))

    def send_up(d):
        return remote(uout.at[d], ubuf.at[t], isend.at[1, d], usem.at[t], s, peer(d))

    send_gain = remote(gain, gother, gsem.at[0], gsem.at[1], other, t)
    send_gain.start()

    @pl.when(level == 0)
    def _():
        for d in range(1, tensors):
            send_hidden(d).start()

    for d in range(1, tensors):
        read_down(d).wait()
        send_down(d).start()
        read_up(d).wait()
        send_up(d).start()

    def send_out(m, c):
        return remote(outbuf.at[m, c], xbuf.at[m, b, c], osend.at[m], ysem.at[m, c], s + 2, t)

    def send_across(m, c):
        return remote(outbuf.at[m, c], xbuf.at[m, b, c], osend.at[m], xsem.at[m, c], other + 2, t)

    def send_both(m, c):
        send_out(m, c).start()
        if c >= chunks - direct:
            send_across(m, c).start()

    def sent(m):
        landed(outbuf.at[m], osend.at[m])
        if direct:
            landed(outbuf.at[m, 0:direct], osend.at[m])

    def write_out(m, c):
        def write(size):
            here = pl.ds(pl.multiple_of(m * rows, 8), size)
            pltpu.make_async_copy(
                outbuf.at[m, c, 0:size], out.at[0, here, at(c * step, step)], wout.at[m]
            ).start()

        if short == rows:
            write(rows)
        elif isinstance(m, int):
            write(short if m == units - 1 else rows)
        else:
            pl.when(m < units - 1)(lambda: write(rows))
            pl.when(m == units - 1)(lambda: write(short))

    def low_sends(slot, ref):
        for side in range(2):
            for d in range(1 - side, tensors):
                remote(ref, ref, lsend.at[slot], lsem.at[slot, b], s if side == 0 else other, peer(d)).start()

    def low_blocks():
        return [2 * peer(d) + (h if side == 0 else 1 - h) for side in range(2) for d in range(1 - side, tensors)]

    for m in range(batch):
        seg = ids[pl.ds(m, 1), :]
        slot = jnp.zeros_like(seg)
        for g in range(segs):
            slot = jnp.where(seg == g, job_ad[seg_job[m, g]], slot)
        square_of = (spread, spread)
        eye = lax.broadcasted_iota(jnp.int32, square_of, 0) == lax.broadcasted_iota(jnp.int32, square_of, 1)
        lanes = jnp.where(eye, jnp.broadcast_to(slot.astype(f32), square_of), 0.0)
        column = jnp.sum(lanes, axis=1, keepdims=True)
        rank = lax.broadcasted_iota(jnp.int32, (spread, ranks), 1) // R
        mask[m * spread : (m + 1) * spread, :] = jnp.where(rank.astype(f32) == column, 1.0, 0.0)
    if short < rows:
        mask[tokens:, :] = jnp.zeros((units * rows - tokens, ranks), f32)

    def adapters():
        own_down.wait()
        own_up.wait()
        for d in range(1, tensors):
            landed(dbuf.at[peer(d)], dsem.at[peer(d)])
            landed(ubuf.at[peer(d)], usem.at[peer(d)])
        who = owner[0]
        down, up = dbuf[0], ubuf[0]
        for k in range(1, tensors):
            down = jnp.where(who == k, dbuf[k], down)
            up = jnp.where(who == k, ubuf[k], up)
        dsel[:, 0:ranks] = down
        dsel[:, ranks:] = jnp.zeros((piece, TILE - ranks), bf16)
        usel[0:ranks, :] = up
        usel[ranks:, :] = jnp.zeros((TILE - ranks, piece), bf16)

    def widen(kept):
        return jnp.concatenate([kept, jnp.zeros((kept.shape[0], TILE - ranks), kept.dtype)], axis=1)

    def first(accs, lows):
        def main(j, begin, end):
            steps = []
            for n, (_, blk) in enumerate(fetches[begin:end]):
                wait = lambda n=n: fetched(begin + n)
                wait.label = "wwait"
                if n == 0:
                    wait()
                else:
                    steps.insert(n * tiles - 2 + n - 1, wait)
                for i in range(tiles):
                    steps.append([
                        (
                            lambda i=i, q=q, blk=blk: w[
                                at(blk * piece + i * TILE, TILE), j * step + q * TILE : j * step + (q + 1) * TILE
                            ],
                            accs[j][q],
                            lambda i=i, blk=blk: xg0[blk * tiles + i],
                        )
                        for q in range(2)
                    ])
            run(steps)

        for j in range(chunks):
            main(j, j, j + 1)
        with jax.named_scope("gainwait"):
            send_gain.wait_recv()
        square = prepare_first(t, 1 - h, sq0[...])
        for d in range(1, tensors):
            with jax.named_scope("hidwait"):
                landed(x0.at[peer(d)], hidsem.at[peer(d)])
            for hh in range(2):
                square = prepare_first(peer(d), hh, square)
        scale = lax.rsqrt(jnp.sum(square, axis=1, keepdims=True) / full + epsilon)

        with jax.named_scope("adapters"):
            adapters()
        steps = []
        for i in range(0, tiles, 2):
            steps.append([
                (
                    lambda i=i, q=q: dsel[(i + q) * TILE : (i + q + 1) * TILE, :],
                    lows[q],
                    lambda i=i, q=q: xg0[b * tiles + i + q],
                )
                for q in range(2)
            ])
        run(steps)
        low = pltpu.matmul_pop(lows[0]) + pltpu.matmul_pop(lows[1])
        lowbuf[b, 0:tokens] = low[:, 0:ranks]
        low_sends(0, lowbuf.at[b, 0:tokens])

        def finish(j):
            run([[
                (
                    lambda q=q: usel[:, j * step + q * TILE : j * step + (q + 1) * TILE],
                    accs[j][q],
                    lambda: kept0[...],
                )
                for q in range(2)
            ]])
            for q in range(2):
              with jax.named_scope('fin'):
                old = x0[t, :, at(h * piece + j * step + q * TILE, TILE)].astype(f32)
                fresh = old + pltpu.matmul_pop(accs[j][q]) * scale
                for m in range(units):
                    size = short if m == units - 1 else rows
                    cols = slice(q * TILE, (q + 1) * TILE)
                    outbuf[m, j, 0:size, cols] = fresh[m * rows : m * rows + size].astype(bf16)
                    if size < rows:
                        outbuf[m, j, size:, cols] = jnp.zeros((rows - size, TILE), bf16)

            @pl.when(jnp.logical_not(last))
            def _():
                send_both(0, j)
            for m in range(units):
                write_out(m, j)

        ready_chunks = min(3, chunks)
        for j in range(ready_chunks):
            main(j, chunks + j * len(rest()), chunks + (j + 1) * len(rest()))
        with jax.named_scope("lowwait"):
            for blk in low_blocks():
                landed(lowbuf.at[blk, 0:tokens], lsem.at[0, blk])
        low = lowbuf[0, 0:tokens]
        for k in range(1, 2 * tensors):
            low = low + lowbuf[k, 0:tokens]
        kept0[...] = widen((low * mask[0:tokens]).astype(bf16))
        for j in range(ready_chunks):
            finish(j)
        for j in range(ready_chunks, chunks):
            main(j, chunks + j * len(rest()), chunks + (j + 1) * len(rest()))
            finish(j)

        @pl.when(jnp.logical_not(last))
        def _():
            for m in range(1, units):
                sent(m - 1)
                for j in range(chunks):
                    send_both(m, j)
            sent(units - 1)

    arrivals = sorted((c + delay, kind, c) for kind, delay in enumerate(DELAYS) for c in range(chunks))
    lead = min(3, inner * chunks - 1)

    def label(name, step):
        step.label = name
        return step

    def later(accs, lows):
        adapters()
        send_gain.wait_recv()
        with jax.named_scope("wrow"):
            for j in range(chunks):
                for blk in range(blocks):
                    weight_rows(j, blk).wait()

        def pieces(kind):
            hh = h if kind < 2 else 1 - h
            gains = gain if kind < 2 else gother
            if kind % 2 == 0:
                return [(t, 2 * t + hh, gains)]
            return [(peer(d), 2 * peer(d) + hh, gains) for d in range(1, tensors)]

        work = [(kind, c) + p for _, kind, c in arrivals for p in pieces(kind)]

        def arrive(m, kind, c, owner_of, blk):
            ref = xbuf.at[m, blk, c]
            if kind == 0:
                landed(ref, ysem.at[m, c])
                if c < chunks - direct:
                    remote(ref, ref, xsend.at[m], xsem.at[m, c], other, t).start()
            elif kind == 2:
                landed(ref, xsem.at[m, c])
            else:
                landed(ref, psem.at[m, owner_of, kind // 2, c])
            if kind % 2 == 0:
                for d in range(1, tensors):
                    remote(ref, ref, fsend.at[m], psem.at[m, t, kind // 2, c], s, peer(d)).start()

        def unit_steps(m):
            here = {"square": jnp.zeros((rows, 128), f32)}
            steps = []

            def prepare(key):
                _, c, owner_of, blk, gains = work[key]
                x = xbuf[m, blk, c].astype(f32)
                here[key] = x * gains[0:1, at(owner_of * piece + c * step, step)].astype(f32)
                for v in range(step // 128):
                    y = x[:, v * 128 : (v + 1) * 128]
                    here["square"] = here["square"] + y * y

            def lhs(key, i):
                return lambda: here[key][:, i * TILE : (i + 1) * TILE]

            def product(key, i, j):
                _, c, _, blk, _ = work[key]
                return [
                    (
                        lambda q=q: w[
                            at(blk * piece + c * step + i * TILE, TILE),
                            j * step + q * TILE : j * step + (q + 1) * TILE,
                        ],
                        accs[j][q],
                        lhs(key, i),
                    )
                    for q in range(2)
                ]

            def low_product(key, i):
                start = work[key][1] * step + i * TILE
                return [
                    (
                        lambda q=q: dsel[start + q * TILE : start + (q + 1) * TILE, :],
                        lows[q],
                        lhs(key, i + q),
                    )
                    for q in range(2)
                ]

            def low_out():
                low = pltpu.matmul_pop(lows[0]) + pltpu.matmul_pop(lows[1])
                lowbuf[b, unit_rows(m), :] = low[:, 0:ranks]
                low_sends(m, lowbuf.at[b, unit_rows(m)])

            def low_in():
                for blk in low_blocks():
                    landed(lowbuf.at[blk, unit_rows(m)], lsem.at[m, blk])
                low = lowbuf[0, unit_rows(m), :]
                for k in range(1, 2 * tensors):
                    low = low + lowbuf[k, unit_rows(m), :]
                here["kept"] = widen(low * mask[unit_rows(m), :])

            def meet(key):
                kind, c, owner_of, blk, _ = work[key]
                found = [lambda: prepare(key)]
                if kind > 0 or c >= early:
                    name = "arr" + "YDXE"[kind] + str(c)
                    found = [label(name, lambda: arrive(m, kind, c, owner_of, blk))] + found
                return found

            def scaling():
                total = jnp.sum(here["square"], axis=1, keepdims=True)
                here["scale"] = lax.rsqrt(total / full + epsilon)

            def leave(j):
                for q in range(2):
                    cols = slice(q * TILE, (q + 1) * TILE)
                    old = xbuf[m, b, j, :, cols].astype(f32)
                    fresh = old + pltpu.matmul_pop(accs[j][q]) * here["scale"]
                    outbuf[m, j, :, cols] = fresh.astype(bf16)

                @pl.when(jnp.logical_not(last))
                def _():
                    send_both(m, j)
                write_out(m, j)
                if j < early:
                    @pl.when(m + 1 < units)
                    def _():
                        arrive(m + 1, 0, j, t, b)

            pending = False
            steps += meet(0)
            tail = len(work) - TAIL
            for key, (kind, c, _, _, _) in enumerate(work[:tail]):
                low_out_at = len(steps) + inner * chunks // 2
                for i in range(inner):
                    for j in range(chunks):
                        steps.append(product(key, i, j))
                if kind == 0:
                    for i in range(0, inner, 2):
                        steps.append(low_product(key, i))
                if pending:
                    steps.insert(low_out_at, label("lowout", low_out))
                pending = kind == 0 and c == chunks - 1
                ahead = meet(key + 1)
                if key + 1 == tail:
                    ahead = [label("lowin", low_in)] + ahead
                    for more in range(tail + 1, len(work)):
                        ahead += meet(more)
                steps[len(steps) - lead : len(steps) - lead] = ahead
            if pending:
                steps.append(low_out)
            for j in range(chunks):
                for key in range(tail, len(work)):
                    for i in range(inner):
                        steps.append(product(key, i, j))
                steps.append([
                    (
                        lambda j=j, q=q: usel[:, j * step + q * TILE : j * step + (q + 1) * TILE],
                        accs[j][q],
                        lambda: here["kept"],
                    )
                    for q in range(2)
                ])
                if j == 0:
                    steps.append(scaling)
                if j > 0:
                    back = len(steps) - max(0, len(products_of(steps[-TAIL * inner - 1 :])) - LAG)
                    steps.insert(back, label("leave", lambda j=j: leave(j - 1)))
            steps.append(label("leave", lambda: leave(chunks - 1)))
            return steps

        begin = products_of(unit_steps(0))
        carried = len(begin) % 2 == 0
        if carried:
            for n in range(2):
                stage(begin[n], n)
        for c in range(early):
            with jax.named_scope("first"):
                arrive(0, 0, c, t, b)

        def unit(m, _):
            run(unit_steps(m), carried)
            return 0

        lax.fori_loop(0, units, unit, 0)
        if carried:
            for n in range(2):
                for q in range(2):
                    pltpu.matmul_acc_lhs(accs[0][q], jnp.zeros((rows, TILE), f32), load_staged_rhs=n)
            for q in range(2):
                pltpu.matmul_pop(accs[0][q])

        for m in range(units):
            if chunks > direct:
                landed(xbuf.at[m, 0, 0 : chunks - direct], xsend.at[m])
            if tensors > 1:
                landed(xbuf.at[m, 0 : 2 * (tensors - 1)], fsend.at[m])
            landed(lowbuf.at[0 : 2 * tensors - 1, m * rows : (m + 1) * rows], lsend.at[m])

    def body(*flat):
        for acc in flat:
            pltpu.matmul_pop(acc)
        pairs = [flat[2 * j : 2 * j + 2] for j in range(2 * chunks + 2)]

        @pl.when(level == 0)
        def _():
            first(pairs[:chunks], pairs[-2])

        @pl.when(level > 0)
        def _():
            later(pairs[chunks:-2], pairs[-1])

    heights = chunks * [tokens] + chunks * [rows] + [tokens, rows]
    pl.run_scoped(body, *[pltpu.ACC(q)((height, TILE), f32) for height in heights for q in range(2)])

    send_gain.wait_send()
    for d in range(1, tensors):
        send_down(d).wait_send()
        send_up(d).wait_send()

    @pl.when(level == 0)
    def _():
        for d in range(1, tensors):
            send_hidden(d).wait_send()
        landed(lowbuf.at[0 : 2 * tensors - 1, 0:tokens], lsend.at[0])

    @pl.when(jnp.logical_not(last) & (level > 0))
    def _():
        for m in range(units):
            sent(m)

    for m in range(units):
        landed(outbuf.at[m, :, 0 : short if m == units - 1 else rows], wout.at[m])


def local(
    hidden_in, segment_ids, segment_job, job_adapter, owner, frozen, norm_gain, inbox_down, inbox_up
):
    tensors = lax.axis_size("tensor")
    sections = lax.axis_size("section")
    batches = segment_ids.shape
    depth, piece = frozen.shape[1:]
    ranks = inbox_down.shape[3]
    step = 2 * TILE
    chunks = piece // step
    tokens = batches[0] * batches[1]
    rows = min(UNIT, tokens)
    units = -(-tokens // rows)
    anywhere = pl.BlockSpec(memory_space=pl.ANY)
    smem = pl.BlockSpec(memory_space=pltpu.SMEM)
    vmem = pl.BlockSpec(memory_space=pltpu.VMEM)
    dma = pltpu.SemaphoreType.DMA
    body = functools.partial(
        kernel, sections, tensors, batches, rows, piece, chunks, ranks,
        (segment_job.shape[1], job_adapter.shape[0]),
    )
    return pl.pallas_call(
        body,
        out_shape=jax.ShapeDtypeStruct((1, tokens, piece), bf16),
        in_specs=[anywhere, vmem, smem, smem, smem, anywhere, vmem, anywhere, anywhere],
        out_specs=anywhere,
        scratch_shapes=[
            pltpu.VMEM((depth, piece), bf16),
            pltpu.VMEM((tensors, tokens, 2 * piece), bf16),
            pltpu.VMEM((depth // TILE, tokens, TILE), bf16),
            pltpu.VMEM((units, 2 * tensors, chunks, rows, step), bf16),
            pltpu.VMEM((units, chunks, rows, step), bf16),
            pltpu.VMEM(norm_gain.shape, bf16),
            pltpu.VMEM((tensors, piece, ranks), bf16),
            pltpu.VMEM((tensors, ranks, piece), bf16),
            pltpu.VMEM((tensors, piece, ranks), bf16),
            pltpu.VMEM((tensors, ranks, piece), bf16),
            pltpu.VMEM((piece, TILE), bf16),
            pltpu.VMEM((TILE, piece), bf16),
            pltpu.VMEM((2 * tensors, units * rows, ranks), f32),
            pltpu.VMEM((units * rows, ranks), f32),
            pltpu.VMEM((tokens, TILE), bf16),
            pltpu.VMEM((tokens, 128), f32),
            dma((chunks, 2 * tensors)),
            dma((tensors,)),
            dma((tensors,)),
            dma((2, tensors)),
            dma((tensors,)),
            dma((tensors,)),
            dma((2, tensors)),
            dma((2,)),
            dma((units, chunks)),
            dma((units, chunks)),
            dma((units, tensors, 2, chunks)),
            dma((units, 2 * tensors)),
            dma((units,)),
            dma((units,)),
            dma((units,)),
            dma((units,)),
            dma((units,)),
        ],
        compiler_params=pltpu.CompilerParams(
            collective_id=0, has_side_effects=True, vmem_limit_bytes=60 * 2**20
        ),
    )(hidden_in, segment_ids, segment_job, job_adapter, owner, frozen, norm_gain, inbox_down, inbox_up)


def solution(mesh):
    mapped = jax.shard_map(
        local,
        mesh=mesh,
        in_specs=(
            P(None, "tensor"),
            P(),
            P(),
            P(),
            P("section"),
            P("section", None, "tensor"),
            P("section", None),
            P("section", "tensor", None, None),
            P("section", "tensor", None, None),
        ),
        out_specs=P("section", None, "tensor"),
        check_vma=False,
    )
    return mapped
```

```python
import functools
import jax
import jax.numpy as jnp
from jax import lax
from jax.experimental import pallas as pl
from jax.experimental.pallas import tpu as pltpu
from jax.sharding import PartitionSpec as P

R = 32
TILE = 256
UNIT = 32
WIDE = False
EARLY = 0
DELAYS = (0, 4, 8, 12)
TAIL = 1
LAG = 4
MESH = pl.DeviceIdType.MESH
epsilon = 1e-05
f32, bf16 = jnp.float32, jnp.bfloat16


def products_of(steps):
    return [step for step in steps if isinstance(step, list)]


def stage(product, n):
    for q, (rhs, _, _) in enumerate(product):
        pltpu.matmul_push_rhs(rhs(), staging_register=n % 2, mxu_index=q)


def run(steps, carried=False):
    products = products_of(steps)
    count = len(products)
    if not carried:
        for n in range(min(2, count)):
            stage(products[n], n)
    n = 0
    for step in steps:
        if isinstance(step, list):
            for _, acc, lhs in step:
                pltpu.matmul_acc_lhs(acc, lhs(), load_staged_rhs=n % 2)
            if n + 2 < count:
                stage(products[n + 2], n)
            elif carried:
                stage(products[n + 2 - count], n)
            n += 1
        else:
            with jax.named_scope(getattr(step, "label", "step")):
                step()


def kernel(
    sections, tensors, batches, rows, piece, chunks, ranks, jobs_of,
    hidden, ids, seg_job, job_ad, owner, frozen, gain, idown, iup,
    out,
    w, x0, xg0, xbuf, outbuf, gother, dout, uout, dbuf, ubuf, dsel, usel, lowbuf, mask, kept0, sq0,
    wsem, hidsem, hidsend, ready, dsem, usem, isend, gsem, ysem, xsem, psem, lsem,
    osend, xsend, fsend, lsend, wout,
):
    levels = sections // 2
    step = piece // chunks
    batch, spread = batches
    tokens = batch * spread
    units = -(-tokens // rows)
    short = tokens - (units - 1) * rows
    full = 2 * tensors * piece
    blocks = 2 * tensors
    inner = step // TILE
    tiles = piece // TILE
    segs, jobs = jobs_of
    window = 6
    early = min(EARLY, chunks - 1)
    s = lax.axis_index("section")
    t = lax.axis_index("tensor")
    h = lax.rem(s, 2)
    level = s // 2
    other = s + 1 - 2 * h
    b = 2 * t + h
    last = level == levels - 1

    def peer(d):
        return lax.rem(t + d, tensors)

    def at(start, size):
        return pl.ds(pl.multiple_of(start, TILE), size)

    def part(k):
        return at(k * piece, piece)

    def remote(src, dst, send, recv, section, tensor):
        return pltpu.make_async_remote_copy(
            src_ref=src, dst_ref=dst, send_sem=send, recv_sem=recv,
            device_id=(section, tensor), device_id_type=MESH,
        )

    def landed(ref, sem):
        pltpu.make_async_copy(ref, ref, sem).wait()

    def unit_rows(m):
        return pl.ds(pl.multiple_of(m * rows, 8), rows)

    own_hidden = pltpu.make_async_copy(hidden, x0.at[t], hidsem.at[t])
    own_down = pltpu.make_async_copy(idown.at[0, 0, part(t), :], dbuf.at[t], dsem.at[t])
    own_up = pltpu.make_async_copy(iup.at[0, 0, :, part(t)], ubuf.at[t], usem.at[t])

    def read_down(d):
        return pltpu.make_async_copy(idown.at[0, 0, part(peer(d)), :], dout.at[d], ready.at[0, d])

    def read_up(d):
        return pltpu.make_async_copy(iup.at[0, 0, :, part(peer(d))], uout.at[d], ready.at[1, d])

    def weight_cols(j, blk):
        here = (part(blk), at(j * step, step))
        return pltpu.make_async_copy(frozen.at[(0,) + here], w.at[here], wsem.at[j, blk])

    def weight_rows(j, blk):
        here = at(blk * piece + j * step, step)
        return pltpu.make_async_copy(frozen.at[0, here, :], w.at[here, :], wsem.at[j, blk])

    def rest():
        return [2 * t + 1 - h] + [2 * peer(d) + hh for d in range(1, tensors) for hh in range(2)]

    barrier = pltpu.get_barrier_semaphore()

    def greet(section, tensor):
        pl.semaphore_signal(barrier, inc=1, device_id=(section, tensor), device_id_type=MESH)

    for d in range(1, tensors):
        greet(s, peer(d))
    for d in range(tensors):
        greet(other, peer(d))

    @pl.when(level > 0)
    def _():
        greet(s - 2, t)

    @pl.when(level < levels - 1)
    def _():
        greet(s + 2, t)

    @pl.when(level == 0)
    def _():
        own_hidden.start()

    def read_adapters():
        own_down.start()
        own_up.start()

    for d in range(1, tensors):
        read_down(d).start()
        read_up(d).start()

    fetches = [(j, b) for j in range(chunks)] + [(j, blk) for j in range(chunks) for blk in rest()]

    def fetch(n):
        if n < len(fetches):
            weight_cols(*fetches[n]).start()

    def fetched(n):
        weight_cols(*fetches[n]).wait()
        fetch(n + window)

    @pl.when(level == 0)
    def _():
        fetch(0)

    @pl.when(level > 0)
    def _():
        read_adapters()
        for j in range(chunks):
            for blk in range(blocks):
                weight_rows(j, blk).start()

    def gain_row(hh, start, size):
        near = gain[0:1, at(start, size)].astype(f32)
        return near if hh is None else jnp.where(h == hh, near, gother[0:1, at(start, size)].astype(f32))

    def prepare_first(owner_of, hh, square):
        blk = 2 * owner_of + (h if hh is None else hh)
        start = (h if hh is None else hh) * piece

        def one(i, square):
            x = x0[owner_of, :, at(start + i * TILE, TILE)].astype(f32)
            xg0[blk * tiles + i] = (x * gain_row(hh, owner_of * piece + i * TILE, TILE)).astype(bf16)
            for v in range(TILE // 128):
                y = x[:, v * 128 : (v + 1) * 128]
                square = square + y * y
            return square

        return lax.fori_loop(0, tiles, one, square)

    @pl.when(level == 0)
    def _():
        own_hidden.wait()
        for n in range(1, 3):
            fetch(n)
        read_adapters()
        for n in range(3, window):
            fetch(n)
        sq0[...] = prepare_first(t, None, jnp.zeros((tokens, 128), f32))

    ends = (level > 0).astype(jnp.int32) + (level < levels - 1).astype(jnp.int32)
    with jax.named_scope("barrier"):
        pl.semaphore_wait(barrier, 2 * tensors - 1 + ends)

    def send_hidden(d):
        return remote(x0.at[t], x0.at[t], hidsend.at[d], hidsem.at[t], s, peer(d))

    def send_down(d):
        return remote(dout.at[d], dbuf.at[t], isend.at[0, d], dsem.at[t], s, peer(d))

    def send_up(d):
        return remote(uout.at[d], ubuf.at[t], isend.at[1, d], usem.at[t], s, peer(d))

    send_gain = remote(gain, gother, gsem.at[0], gsem.at[1], other, t)
    send_gain.start()

    @pl.when(level == 0)
    def _():
        for d in range(1, tensors):
            send_hidden(d).start()

    for d in range(1, tensors):
        read_down(d).wait()
        send_down(d).start()
        read_up(d).wait()
        send_up(d).start()

    def send_out(m, c, i):
        return remote(outbuf.at[m, c, i], xbuf.at[m, b, c, i], osend.at[m], ysem.at[m, c, i], s + 2, t)

    def send_next(m, c):
        for i in range(inner):
            send_out(m, c, i).start()

    def sent(m):
        landed(outbuf.at[m], osend.at[m])

    def write_out(m, c):
        def write(size):
            here = pl.ds(pl.multiple_of(m * rows, 8), size)
            for i in range(inner):
                pltpu.make_async_copy(
                    outbuf.at[m, c, i, 0:size], out.at[0, here, at(c * step + i * TILE, TILE)], wout.at[m]
                ).start()

        if short == rows:
            write(rows)
        elif isinstance(m, int):
            write(short if m == units - 1 else rows)
        else:
            pl.when(m < units - 1)(lambda: write(rows))
            pl.when(m == units - 1)(lambda: write(short))

    def low_sends(slot, ref):
        for side in range(2):
            for d in range(1 - side, tensors):
                remote(ref, ref, lsend.at[slot], lsem.at[slot, b], s if side == 0 else other, peer(d)).start()

    def low_blocks():
        return [2 * peer(d) + (h if side == 0 else 1 - h) for side in range(2) for d in range(1 - side, tensors)]

    for m in range(batch):
        seg = ids[pl.ds(m, 1), :]
        slot = jnp.zeros_like(seg)
        for g in range(segs):
            slot = jnp.where(seg == g, job_ad[seg_job[m, g]], slot)
        square_of = (spread, spread)
        eye = lax.broadcasted_iota(jnp.int32, square_of, 0) == lax.broadcasted_iota(jnp.int32, square_of, 1)
        lanes = jnp.where(eye, jnp.broadcast_to(slot.astype(f32), square_of), 0.0)
        column = jnp.sum(lanes, axis=1, keepdims=True)
        rank = lax.broadcasted_iota(jnp.int32, (spread, ranks), 1) // R
        mask[m * spread : (m + 1) * spread, :] = jnp.where(rank.astype(f32) == column, 1.0, 0.0)
    if short < rows:
        mask[tokens:, :] = jnp.zeros((units * rows - tokens, ranks), f32)

    def adapters():
        own_down.wait()
        own_up.wait()
        for d in range(1, tensors):
            landed(dbuf.at[peer(d)], dsem.at[peer(d)])
            landed(ubuf.at[peer(d)], usem.at[peer(d)])
        who = owner[0]
        down, up = dbuf[0], ubuf[0]
        for k in range(1, tensors):
            down = jnp.where(who == k, dbuf[k], down)
            up = jnp.where(who == k, ubuf[k], up)
        dsel[:, 0:ranks] = down
        dsel[:, ranks:] = jnp.zeros((piece, TILE - ranks), bf16)
        usel[0:ranks, :] = up
        usel[ranks:, :] = jnp.zeros((TILE - ranks, piece), bf16)

    def widen(kept):
        return jnp.concatenate([kept, jnp.zeros((kept.shape[0], TILE - ranks), kept.dtype)], axis=1)

    def first(accs, lows):
        def main(j, begin, end):
            steps = []
            for n, (_, blk) in enumerate(fetches[begin:end]):
                wait = lambda n=n: fetched(begin + n)
                wait.label = "wwait"
                if n == 0:
                    wait()
                else:
                    steps.insert(n * tiles - 2 + n - 1, wait)
                for i in range(tiles):
                    steps.append([
                        (
                            lambda i=i, q=q, blk=blk: w[
                                at(blk * piece + i * TILE, TILE), j * step + q * TILE : j * step + (q + 1) * TILE
                            ],
                            accs[j][q],
                            lambda i=i, blk=blk: xg0[blk * tiles + i],
                        )
                        for q in range(2)
                    ])
            run(steps)

        for j in range(chunks):
            main(j, j, j + 1)
        with jax.named_scope("gainwait"):
            send_gain.wait_recv()
        square = prepare_first(t, 1 - h, sq0[...])
        for d in range(1, tensors):
            with jax.named_scope("hidwait"):
                landed(x0.at[peer(d)], hidsem.at[peer(d)])
            for hh in range(2):
                square = prepare_first(peer(d), hh, square)
        scale = lax.rsqrt(jnp.sum(square, axis=1, keepdims=True) / full + epsilon)

        with jax.named_scope("adapters"):
            adapters()
        steps = []
        for i in range(0, tiles, 2):
            steps.append([
                (
                    lambda i=i, q=q: dsel[(i + q) * TILE : (i + q + 1) * TILE, :],
                    lows[q],
                    lambda i=i, q=q: xg0[b * tiles + i + q],
                )
                for q in range(2)
            ])
        run(steps)
        low = pltpu.matmul_pop(lows[0]) + pltpu.matmul_pop(lows[1])
        lowbuf[b, 0:tokens] = low[:, 0:ranks]
        low_sends(0, lowbuf.at[b, 0:tokens])

        def finish(j):
            run([[
                (
                    lambda q=q: usel[:, j * step + q * TILE : j * step + (q + 1) * TILE],
                    accs[j][q],
                    lambda: kept0[...],
                )
                for q in range(2)
            ]])
            for q in range(2):
              with jax.named_scope('fin'):
                old = x0[t, :, at(h * piece + j * step + q * TILE, TILE)].astype(f32)
                fresh = old + pltpu.matmul_pop(accs[j][q]) * scale
                for m in range(units):
                    size = short if m == units - 1 else rows
                    outbuf[m, j, q, 0:size] = fresh[m * rows : m * rows + size].astype(bf16)
                    if size < rows:
                        outbuf[m, j, q, size:] = jnp.zeros((rows - size, TILE), bf16)

            @pl.when(jnp.logical_not(last))
            def _():
                send_next(0, j)
            for m in range(units):
                write_out(m, j)

        ready_chunks = min(3, chunks)
        for j in range(ready_chunks):
            main(j, chunks + j * len(rest()), chunks + (j + 1) * len(rest()))
        with jax.named_scope("lowwait"):
            for blk in low_blocks():
                landed(lowbuf.at[blk, 0:tokens], lsem.at[0, blk])
        low = lowbuf[0, 0:tokens]
        for k in range(1, 2 * tensors):
            low = low + lowbuf[k, 0:tokens]
        kept0[...] = widen((low * mask[0:tokens]).astype(bf16))
        for j in range(ready_chunks):
            finish(j)
        for j in range(ready_chunks, chunks):
            main(j, chunks + j * len(rest()), chunks + (j + 1) * len(rest()))
            finish(j)

        @pl.when(jnp.logical_not(last))
        def _():
            for m in range(1, units):
                sent(m - 1)
                for j in range(chunks):
                    send_next(m, j)
            sent(units - 1)

    arrivals = sorted((c + delay, kind, c) for kind, delay in enumerate(DELAYS) for c in range(chunks))
    lead = min(1, inner * chunks - 1)

    def label(name, step):
        step.label = name
        return step

    def later(accs, lows):
        adapters()
        send_gain.wait_recv()
        with jax.named_scope("wrow"):
            for j in range(chunks):
                for blk in range(blocks):
                    weight_rows(j, blk).wait()

        def pieces(kind):
            hh = h if kind < 2 else 1 - h
            gains = gain if kind < 2 else gother
            if kind % 2 == 0:
                return [(t, 2 * t + hh, gains)]
            return [(peer(d), 2 * peer(d) + hh, gains) for d in range(1, tensors)]

        work = [(kind, c) + p for _, kind, c in arrivals for p in pieces(kind)]

        def arrive(m, kind, c, owner_of, blk):
            for i in range(inner):
                ref = xbuf.at[m, blk, c, i]
                if kind == 0:
                    landed(ref, ysem.at[m, c, i])
                    remote(ref, ref, xsend.at[m], xsem.at[m, c, i], other, t).start()
                elif kind == 2:
                    landed(ref, xsem.at[m, c, i])
                else:
                    landed(ref, psem.at[m, owner_of, kind // 2, c, i])
                if kind % 2 == 0:
                    for d in range(1, tensors):
                        remote(ref, ref, fsend.at[m], psem.at[m, t, kind // 2, c, i], s, peer(d)).start()

        def unit_steps(m):
            here = {"square": jnp.zeros((rows, 128), f32)}
            steps = []

            def prepare(key):
                _, c, owner_of, blk, gains = work[key]
                here[key] = []
                for i in range(inner):
                    x = xbuf[m, blk, c, i].astype(f32)
                    g = gains[0:1, at(owner_of * piece + c * step + i * TILE, TILE)].astype(f32)
                    here[key].append((x * g).astype(bf16) if WIDE else x * g)
                    for v in range(TILE // 128):
                        y = x[:, v * 128 : (v + 1) * 128]
                        here["square"] = here["square"] + y * y

            def lhs(key, i):
                return lambda: here[key][i]

            def product(key, i, j):
                _, c, _, blk, _ = work[key]
                return [
                    (
                        lambda q=q: w[
                            at(blk * piece + c * step + i * TILE, TILE),
                            j * step + q * TILE : j * step + (q + 1) * TILE,
                        ],
                        accs[j][q],
                        lhs(key, i),
                    )
                    for q in range(2)
                ]

            def low_product(key, i):
                start = work[key][1] * step + i * TILE
                return [
                    (
                        lambda q=q: dsel[start + q * TILE : start + (q + 1) * TILE, :],
                        lows[q],
                        lhs(key, i + q),
                    )
                    for q in range(2)
                ]

            def low_out():
                low = pltpu.matmul_pop(lows[0]) + pltpu.matmul_pop(lows[1])
                lowbuf[b, unit_rows(m), :] = low[:, 0:ranks]
                low_sends(m, lowbuf.at[b, unit_rows(m)])

            def low_in():
                for blk in low_blocks():
                    landed(lowbuf.at[blk, unit_rows(m)], lsem.at[m, blk])
                low = lowbuf[0, unit_rows(m), :]
                for k in range(1, 2 * tensors):
                    low = low + lowbuf[k, unit_rows(m), :]
                here["kept"] = widen(low * mask[unit_rows(m), :])

            def meet(key):
                kind, c, owner_of, blk, _ = work[key]
                found = [lambda: prepare(key)]
                if kind > 0 or c >= early:
                    name = "arr" + "YDXE"[kind] + str(c)
                    found = [label(name, lambda: arrive(m, kind, c, owner_of, blk))] + found
                return found

            def scaling():
                total = jnp.sum(here["square"], axis=1, keepdims=True)
                here["scale"] = lax.rsqrt(total / full + epsilon)

            def leave(j):
                for q in range(2):
                    old = xbuf[m, b, j, q].astype(f32)
                    fresh = old + pltpu.matmul_pop(accs[j][q]) * here["scale"]
                    outbuf[m, j, q] = fresh.astype(bf16)

                @pl.when(jnp.logical_not(last))
                def _():
                    send_next(m, j)
                write_out(m, j)
                if j < early:
                    @pl.when(m + 1 < units)
                    def _():
                        arrive(m + 1, 0, j, t, b)

            pending = False
            steps += meet(0)
            tail = len(work) - TAIL
            for key, (kind, c, _, _, _) in enumerate(work[:tail]):
                low_out_at = len(steps) + inner * chunks // 2
                for i in range(inner):
                    for j in range(chunks):
                        steps.append(product(key, i, j))
                if kind == 0:
                    for i in range(0, inner, 2):
                        steps.append(low_product(key, i))
                if pending:
                    steps.insert(low_out_at, label("lowout", low_out))
                pending = kind == 0 and c == chunks - 1
                ahead = meet(key + 1)
                if key + 1 == tail:
                    ahead = [label("lowin", low_in)] + ahead
                    for more in range(tail + 1, len(work)):
                        ahead += meet(more)
                steps[len(steps) - lead : len(steps) - lead] = ahead
            if pending:
                steps.append(low_out)
            for j in range(chunks):
                for key in range(tail, len(work)):
                    for i in range(inner):
                        steps.append(product(key, i, j))
                steps.append([
                    (
                        lambda j=j, q=q: usel[:, j * step + q * TILE : j * step + (q + 1) * TILE],
                        accs[j][q],
                        lambda: here["kept"],
                    )
                    for q in range(2)
                ])
                if j == 0:
                    steps.append(scaling)
                if j > 0:
                    back = len(steps) - max(0, len(products_of(steps[-TAIL * inner - 1 :])) - LAG)
                    steps.insert(back, label("leave", lambda j=j: leave(j - 1)))
            steps.append(label("leave", lambda: leave(chunks - 1)))
            return steps

        begin = products_of(unit_steps(0))
        carried = len(begin) % 2 == 0
        if carried:
            for n in range(2):
                stage(begin[n], n)
        for c in range(early):
            with jax.named_scope("first"):
                arrive(0, 0, c, t, b)

        def unit(m, _):
            run(unit_steps(m), carried)
            return 0

        lax.fori_loop(0, units, unit, 0)
        if carried:
            for n in range(2):
                for q in range(2):
                    pltpu.matmul_acc_lhs(accs[0][q], jnp.zeros((rows, TILE), f32), load_staged_rhs=n)
            for q in range(2):
                pltpu.matmul_pop(accs[0][q])

        for m in range(units):
            landed(xbuf.at[m, 0], xsend.at[m])
            if tensors > 1:
                landed(xbuf.at[m, 0 : 2 * (tensors - 1)], fsend.at[m])
            landed(lowbuf.at[0 : 2 * tensors - 1, m * rows : (m + 1) * rows], lsend.at[m])

    def body(*flat):
        for acc in flat:
            pltpu.matmul_pop(acc)
        pairs = [flat[2 * j : 2 * j + 2] for j in range(2 * chunks + 2)]

        @pl.when(level == 0)
        def _():
            first(pairs[:chunks], pairs[-2])

        @pl.when(level > 0)
        def _():
            later(pairs[chunks:-2], pairs[-1])

    heights = chunks * [tokens] + chunks * [rows] + [tokens, rows]
    pl.run_scoped(body, *[pltpu.ACC(q)((height, TILE), f32) for height in heights for q in range(2)])

    send_gain.wait_send()
    for d in range(1, tensors):
        send_down(d).wait_send()
        send_up(d).wait_send()

    @pl.when(level == 0)
    def _():
        for d in range(1, tensors):
            send_hidden(d).wait_send()
        landed(lowbuf.at[0 : 2 * tensors - 1, 0:tokens], lsend.at[0])

    @pl.when(jnp.logical_not(last) & (level > 0))
    def _():
        for m in range(units):
            sent(m)

    for m in range(units):
        landed(outbuf.at[m, :, :, 0 : short if m == units - 1 else rows], wout.at[m])


def local(
    hidden_in, segment_ids, segment_job, job_adapter, owner, frozen, norm_gain, inbox_down, inbox_up
):
    tensors = lax.axis_size("tensor")
    sections = lax.axis_size("section")
    batches = segment_ids.shape
    depth, piece = frozen.shape[1:]
    ranks = inbox_down.shape[3]
    step = 2 * TILE
    chunks = piece // step
    inner = step // TILE
    tokens = batches[0] * batches[1]
    rows = min(UNIT, tokens)
    units = -(-tokens // rows)
    anywhere = pl.BlockSpec(memory_space=pl.ANY)
    smem = pl.BlockSpec(memory_space=pltpu.SMEM)
    vmem = pl.BlockSpec(memory_space=pltpu.VMEM)
    dma = pltpu.SemaphoreType.DMA
    body = functools.partial(
        kernel, sections, tensors, batches, rows, piece, chunks, ranks,
        (segment_job.shape[1], job_adapter.shape[0]),
    )
    return pl.pallas_call(
        body,
        out_shape=jax.ShapeDtypeStruct((1, tokens, piece), bf16),
        in_specs=[anywhere, vmem, smem, smem, smem, anywhere, vmem, anywhere, anywhere],
        out_specs=anywhere,
        scratch_shapes=[
            pltpu.VMEM((depth, piece), bf16),
            pltpu.VMEM((tensors, tokens, 2 * piece), bf16),
            pltpu.VMEM((depth // TILE, tokens, TILE), bf16),
            pltpu.VMEM((units, 2 * tensors, chunks, inner, rows, TILE), bf16),
            pltpu.VMEM((units, chunks, inner, rows, TILE), bf16),
            pltpu.VMEM(norm_gain.shape, bf16),
            pltpu.VMEM((tensors, piece, ranks), bf16),
            pltpu.VMEM((tensors, ranks, piece), bf16),
            pltpu.VMEM((tensors, piece, ranks), bf16),
            pltpu.VMEM((tensors, ranks, piece), bf16),
            pltpu.VMEM((piece, TILE), bf16),
            pltpu.VMEM((TILE, piece), bf16),
            pltpu.VMEM((2 * tensors, units * rows, ranks), f32),
            pltpu.VMEM((units * rows, ranks), f32),
            pltpu.VMEM((tokens, TILE), bf16),
            pltpu.VMEM((tokens, 128), f32),
            dma((chunks, 2 * tensors)),
            dma((tensors,)),
            dma((tensors,)),
            dma((2, tensors)),
            dma((tensors,)),
            dma((tensors,)),
            dma((2, tensors)),
            dma((2,)),
            dma((units, chunks, inner)),
            dma((units, chunks, inner)),
            dma((units, tensors, 2, chunks, inner)),
            dma((units, 2 * tensors)),
            dma((units,)),
            dma((units,)),
            dma((units,)),
            dma((units,)),
            dma((units,)),
        ],
        compiler_params=pltpu.CompilerParams(
            collective_id=0, has_side_effects=True, vmem_limit_bytes=60 * 2**20
        ),
    )(hidden_in, segment_ids, segment_job, job_adapter, owner, frozen, norm_gain, inbox_down, inbox_up)


def solution(mesh):
    mapped = jax.shard_map(
        local,
        mesh=mesh,
        in_specs=(
            P(None, "tensor"),
            P(),
            P(),
            P(),
            P("section"),
            P("section", None, "tensor"),
            P("section", None),
            P("section", "tensor", None, None),
            P("section", "tensor", None, None),
        ),
        out_specs=P("section", None, "tensor"),
        check_vma=False,
    )
    return mapped
```
